32 devices in a mesh: dp: 8 (over y, x, core), expert: 4 (over z).
Axes of the slice: x: 2, y: 2, z: 4, core: 2. Of those that a mesh axis runs over, the one named last changes fastest.
Arguments:
- tokens: bfloat16 [18912, 512], P(('dp', 'expert')), may hold values from -6 to 6
- cotangent: float32 [18912, 512], P(('dp', 'expert')), may hold values from -6 to 6
- dense_gains: float32 [2, 512], replicated, may hold values from 0.1 to 1.9
- dense_shifts: float32 [2, 512], replicated, may hold values from -1.75 to 1.75
- dense_qkv: bfloat16 [512, 1536], replicated, may hold values from -0.25 to 0.25
- dense_biases: float32 [4, 512], replicated, may hold values from -3 to 3
- dense_proj: bfloat16 [512, 512], replicated, may hold values from -1 to 1
- dense_up: bfloat16 [512, 2048], replicated, may hold values from -0.25 to 0.25
- dense_up_bias: float32 [2048], replicated, may hold values from -3 to 3
- dense_down: bfloat16 [2048, 512], replicated, may hold values from -0.125 to 0.125
- moe_gains: float32 [2, 512], replicated, may hold values from 0.1 to 1.9
- moe_shifts: float32 [2, 512], replicated, may hold values from -1.75 to 1.75
- moe_qkv: bfloat16 [512, 1536], replicated, may hold values from -0.25 to 0.25
- moe_biases: float32 [3, 512], replicated, may hold values from -3 to 3
- moe_proj: bfloat16 [512, 512], replicated, may hold values from -1 to 1
- router: bfloat16 [512, 8], replicated, may hold values from -0.25 to 0.25
- router_noise: float32 [18912, 8], P(('dp', 'expert')), may hold values from -6 to 6
- routes: int32 [18912, 2], P(('dp', 'expert')), may hold values from 0 to 7, all different within a row; in each aligned block of 591 rows (0 to 590, 591 to 1181, ...) at most 185 rows name the same one
- expert_in: bfloat16 [8, 512, 2048], P('expert'), may hold values from -0.25 to 0.25
- expert_in_bias: float32 [8, 2048], P('expert'), may hold values from -3 to 3
- expert_out: bfloat16 [8, 2048, 512], P('expert'), may hold values from -2 to 2
- expert_out_bias: float32 [8, 512], P('expert'), may hold values from -3 to 3
Outputs:
- out_tokens: bfloat16 [18912, 512], P(('dp', 'expert'))
- token_grad: float32 [18912, 512], P(('dp', 'expert'))
- dense_gains_grad: float32 [2, 512], P(None, 'dp')
- dense_shifts_grad: float32 [2, 512], P(None, 'dp')
- dense_qkv_grad: float32 [512, 1536], P('dp')
- dense_biases_grad: float32 [4, 512], P(None, 'dp')
- dense_proj_grad: float32 [512, 512], P('dp')
- dense_up_grad: float32 [512, 2048], P('dp')
- dense_up_bias_grad: float32 [2048], P('dp')
- dense_down_grad: float32 [2048, 512], P('dp')
- moe_gains_grad: float32 [2, 512], P(None, 'dp')
- moe_shifts_grad: float32 [2, 512], P(None, 'dp')
- moe_qkv_grad: float32 [512, 1536], P('dp')
- moe_biases_grad: float32 [3, 512], P(None, 'dp')
- moe_proj_grad: float32 [512, 512], P('dp')
- router_grad: float32 [512, 8], P('dp')
- expert_in_grad: float32 [8, 512, 2048], P('expert', 'dp')
- expert_in_bias_grad: float32 [8, 2048], P('expert', 'dp')
- expert_out_grad: float32 [8, 2048, 512], P('expert', 'dp')
- expert_out_bias_grad: float32 [8, 512], P('expert', 'dp')
The draws below stay inside these ranges and needn't reach their ends.
Inputs may be any that keep to these rules, and one draw needn't show every extreme that they name: `routes`: each row names 2 different experts. Among the rows of one device (591 aligned rows) no expert is named by more than 185 rows, and in some devices' rows one expert is named by exactly 185.
All inputs are finite; a program needn't handle non-finite values.
Results may differ from the reference program's by a relative error of at most 0.022.
Values may be sent and summed in bfloat16 or wider, within the bound.
A program may use at most 256 MiB of HBM per device.

```python
import math
import jax
import jax.numpy as jnp
import numpy as np
from jax import lax

D = 512
HEADS = 8
HEAD_DIM = 64
FF = 2048
TOP = 2
SEQ = 197
EXPERTS = 8
TOK_DEV = 591
TOKENS = 18912
CAP = 185


def levels(rng, dims, cuts, least, top_value):
    def one(dim, parts):
        steps = jax.random.uniform(jax.random.fold_in(jax.random.fold_in(rng, 6), dim), (parts,), jnp.float32, least / len(cuts), top_value / len(cuts))
        return jnp.repeat(jnp.exp(steps), dims[dim] // parts).reshape((-1,) + (1,) * (len(dims) - dim - 1))

    factor_of = one(*cuts[0])
    for cut in cuts[1:]:
        factor_of = factor_of * one(*cut)
    return factor_of


def routed_block(rng, own, number, rows, count, top, limit, lean):
    order = jax.random.permutation(rng, count)
    crowded, ordinary = portions_of(count, rows * top, limit, lean, True), portions_of(count, rows * top, limit, lean, False)
    places = jnp.arange(count)

    def named(sizes, rotation):
        used = int((sizes > 0).sum())
        fixed = max(1, used // 4)
        passed = fixed + (places - fixed + rotation * (used - fixed)) % max(1, count - fixed)
        return jnp.zeros((count,), jnp.int32).at[order[jnp.where(places < fixed, places, passed)]].set(jnp.asarray(sizes, jnp.int32))

    sizes = jnp.where(number % 4 == 0, named(crowded, number // 4), named(ordinary, number - number // 4 - 1))
    mixed = jax.random.permutation(jax.random.fold_in(own, 3), count)
    donor, receiver = mixed[0:count // 2 * 2:2], mixed[1:count // 2 * 2:2]
    room = jnp.minimum(sizes[donor] - 1, limit - sizes[receiver]) // 2
    room = jnp.where((donor == order[0]) | (receiver == order[0]) | (sizes[receiver] == 0), 0, jnp.maximum(room, 0))
    passed = jax.random.randint(jax.random.fold_in(own, 4), (count // 2,), 0, 1 << 20) % (room + 1)
    sizes = sizes.at[donor].add(-passed).at[receiver].add(passed)
    labels = jnp.searchsorted(jnp.cumsum(sizes), jnp.arange(rows * top), side="right").astype(jnp.int32)
    table = labels.reshape(top, rows).T
    table = table[jax.random.permutation(jax.random.fold_in(own, 1), rows)]
    rotation = jax.random.randint(jax.random.fold_in(own, 2), (rows, 1), 0, top)
    return jnp.take_along_axis(table, (jnp.arange(top)[None, :] + rotation) % top, axis=1)


def portions_of(number_of, total, bound, skew, full):
    weights = [(1 << 20) // math.isqrt(grade ** skew) + 1 for grade in range(1, number_of + 1)]
    largest = bound if full else min(bound, max(-(-total // number_of), total * weights[0] // sum(weights)))
    least = 1 if total - largest >= number_of - 1 else 0
    counts, surplus = [largest] + [least] * (number_of - 1), total - largest - least * (number_of - 1)
    while surplus > 0:
        movable = [i for i in range(1, number_of) if counts[i] < largest] or [i for i in range(1, number_of) if counts[i] < bound]
        mass, budget = sum([weights[i] for i in movable]), surplus
        for i in movable:
            more = min(bound - counts[i], max(1, budget * weights[i] // mass), surplus)
            counts[i] = counts[i] + more
            surplus = surplus - more
    return np.array(counts)


def gaussian(stream_key, extent, width, most, cuts=(), kind=jnp.bfloat16):
    array = width * jax.random.normal(stream_key, extent, jnp.float32)
    if cuts:
        array = array * levels(stream_key, extent, cuts, -0.22, 0.18)
    return jnp.clip(array, -most, most).astype(kind)


def setup_inputs(seed: int = 0) -> dict:
    arg_keys = jax.random.split(jax.random.key(seed), 23)
    tokens = gaussian(arg_keys[0], (TOKENS, D), 1.0, 6.0, ((0, 32),))
    cotangent = gaussian(arg_keys[1], (TOKENS, D), 1.0, 6.0, ((0, 32),), jnp.float32)
    dense_gains = jnp.clip(1.0 + 0.18 * jax.random.normal(arg_keys[2], (2, D), jnp.float32), 0.1, 1.9)
    dense_shifts = gaussian(arg_keys[3], (2, D), 0.3, 1.75, (), jnp.float32)
    dense_qkv = gaussian(arg_keys[4], (D, 3 * D), D ** -0.5, 0.25)
    dense_biases = gaussian(arg_keys[5], (4, D), 0.5, 3.0, (), jnp.float32)
    dense_proj = gaussian(arg_keys[6], (D, D), (D // 16) ** -0.5, 1.0)
    dense_up = gaussian(arg_keys[7], (D, FF), D ** -0.5, 0.25)
    dense_up_bias = gaussian(arg_keys[8], (FF,), 0.5, 3.0, (), jnp.float32)
    dense_down = gaussian(arg_keys[9], (FF, D), FF ** -0.5, 0.125)
    moe_gains = jnp.clip(1.0 + 0.18 * jax.random.normal(arg_keys[10], (2, D), jnp.float32), 0.1, 1.9)
    moe_shifts = gaussian(arg_keys[11], (2, D), 0.3, 1.75, (), jnp.float32)
    moe_qkv = gaussian(arg_keys[12], (D, 3 * D), D ** -0.5, 0.25)
    moe_biases = gaussian(arg_keys[13], (3, D), 0.5, 3.0, (), jnp.float32)
    moe_proj = gaussian(arg_keys[14], (D, D), (D // 16) ** -0.5, 1.0)
    router = gaussian(arg_keys[15], (D, EXPERTS), D ** -0.5, 0.25)
    router_noise = gaussian(arg_keys[16], (TOKENS, EXPERTS), 1.0, 6.0, ((0, 32),), jnp.float32)
    routes_keys = jax.random.split(jax.random.fold_in(arg_keys[17], 1), TOKENS // TOK_DEV)
    routes_turns = jax.random.permutation(jax.random.fold_in(arg_keys[17], 3), TOKENS // TOK_DEV)
    routes = jax.vmap(lambda own, number: routed_block(jax.random.fold_in(arg_keys[17], 2), own, number, TOK_DEV, EXPERTS, TOP, CAP, 1))(routes_keys, routes_turns).reshape((TOKENS, TOP))
    expert_in = gaussian(arg_keys[18], (EXPERTS, D, FF), D ** -0.5, 0.25, ((0, 4),))
    expert_in_bias = gaussian(arg_keys[19], (EXPERTS, FF), 0.5, 3.0, ((0, 4),), jnp.float32)
    expert_out = gaussian(arg_keys[20], (EXPERTS, FF, D), (max(1, FF // 256)) ** -0.5, 2.0, ((0, 4),))
    expert_out_bias = gaussian(arg_keys[21], (EXPERTS, D), 0.5, 3.0, ((0, 4),), jnp.float32)
    return {"tokens": tokens, "cotangent": cotangent, "dense_gains": dense_gains, "dense_shifts": dense_shifts, "dense_qkv": dense_qkv, "dense_biases": dense_biases, "dense_proj": dense_proj, "dense_up": dense_up, "dense_up_bias": dense_up_bias, "dense_down": dense_down, "moe_gains": moe_gains, "moe_shifts": moe_shifts, "moe_qkv": moe_qkv, "moe_biases": moe_biases, "moe_proj": moe_proj, "router": router, "router_noise": router_noise, "routes": routes, "expert_in": expert_in, "expert_in_bias": expert_in_bias, "expert_out": expert_out, "expert_out_bias": expert_out_bias}


@jax.custom_vjp
def low(v):
    return lax.optimization_barrier(v.astype(jnp.bfloat16)).astype(jnp.float32)

@jax.custom_vjp
def low_back(v):
    return v

def low_keep(v):
    return (low(v), None)

def low_pass(kept, grad):
    return (grad,)

def back_keep(v):
    return (v, None)

def back_low(kept, grad):
    return (low(grad),)
low.defvjp(low_keep, low_pass)
low_back.defvjp(back_keep, back_low)

def matmul(left, right):
    return jnp.dot(left, right, precision=lax.Precision.HIGHEST)

def layer_norm(values, gain, shift):
    average = lax.optimization_barrier(jnp.mean(values, axis=-1, keepdims=True))
    centered = values - average
    variance = lax.optimization_barrier(jnp.mean(centered * centered, axis=-1, keepdims=True))
    return centered * lax.rsqrt(variance + 1e-06) * gain + shift

def attention_part(stream, gain_rows, shifts, qkv_weight, biases, proj_weight):
    normed = low(layer_norm(stream, gain_rows[0], shifts[0]))
    joined = matmul(normed, qkv_weight)
    queries = low_back(low(joined[..., :D] + biases[0]))
    key_rows = low_back(low(joined[..., D:2 * D]))
    values = low_back(low(joined[..., 2 * D:] + biases[1]))
    shaped = stream.shape[:2] + (HEADS, HEAD_DIM)
    scores = jnp.einsum('bqhd,bkhd->bhqk', queries.reshape(shaped), key_rows.reshape(shaped), precision=lax.Precision.HIGHEST) * HEAD_DIM ** (-0.5)
    scores = low_back(scores)
    weights = jax.nn.softmax(scores, axis=-1)
    mixed = jnp.einsum('bhqk,bkhd->bqhd', low(weights), values.reshape(shaped), precision=lax.Precision.HIGHEST)
    mixed = low_back(low(mixed.reshape(stream.shape)))
    branch = low_back(matmul(mixed, proj_weight) + biases[2])
    return stream + branch

def mlp_part(stream, gain_rows, shifts, in_weight, in_bias, out_weight, out_bias):
    normed = low(layer_norm(stream, gain_rows[1], shifts[1]))
    before = low_back(matmul(normed, in_weight) + in_bias)
    hidden = low(jax.nn.gelu(before, approximate=True))
    return stream + low_back(matmul(hidden, out_weight) + out_bias)

def routing_tables(routes):
    blocks = TOKENS // TOK_DEV
    chosen = routes.reshape(blocks, TOK_DEV * TOP)
    onehot = (chosen[:, :, None] == jnp.arange(EXPERTS, dtype=jnp.int32)[None, None, :]).astype(jnp.int32)
    running = jnp.cumsum(onehot, axis=1).astype(jnp.int32) - 1
    slot_index = lax.optimization_barrier(jnp.sum(running * onehot, axis=-1)).astype(jnp.int32)
    block_ids = jnp.arange(blocks, dtype=jnp.int32)[:, None]
    position = (chosen * blocks + block_ids) * CAP + slot_index
    token_ids = block_ids * TOK_DEV + jnp.arange(TOK_DEV * TOP, dtype=jnp.int32)[None, :] // TOP
    table = jnp.full((EXPERTS * blocks * CAP,), TOKENS, jnp.int32)
    table = table.at[position.reshape(-1)].set(token_ids.reshape(-1).astype(jnp.int32))
    return (table.reshape(EXPERTS, blocks * CAP), position.reshape(TOKENS, TOP).astype(jnp.int32))

def reference(tokens, cotangent, dense_gains, dense_shifts, dense_qkv, dense_biases, dense_proj, dense_up, dense_up_bias, dense_down, moe_gains, moe_shifts, moe_qkv, moe_biases, moe_proj, router, router_noise, routes, expert_in, expert_in_bias, expert_out, expert_out_bias):
    table, position = routing_tables(routes)
    noise_values = router_noise.astype(jnp.float32)

    def forward(stream, weights):
        gains_one, shifts_one, qkv_one, biases_one, proj_one, up_weight, up_bias, down_weight, gains_two, shifts_two, qkv_two, biases_two, proj_two, router_weight, expert_up, expert_up_bias, expert_down, expert_down_bias = weights
        images = stream.reshape(TOKENS // (16 * SEQ), 16, SEQ, D)

        def first_layer(group):
            middle = attention_part(group, gains_one, shifts_one, qkv_one, biases_one, proj_one)
            return mlp_part(middle, gains_one, shifts_one, up_weight, up_bias, down_weight, biases_one[3])

        def second_attention(group):
            return attention_part(group, gains_two, shifts_two, qkv_two, biases_two, proj_two)
        after_first = lax.map(jax.checkpoint(first_layer), images)
        after_attn = lax.map(jax.checkpoint(second_attention), after_first).reshape(TOKENS, D)
        normed = low(layer_norm(after_attn, gains_two[1], shifts_two[1]))
        logits = matmul(normed, router_weight) + noise_values
        expert_probs = jax.nn.softmax(logits, axis=-1)
        padded = jnp.concatenate([normed, jnp.zeros((1, D), jnp.float32)], axis=0)

        def one_expert(packed):
            rows_index, in_matrix, in_vector, out_matrix, out_vector = packed
            rows = low_back(padded[rows_index])
            before = low_back(matmul(rows, in_matrix) + in_vector)
            hidden = low(jax.nn.gelu(before, approximate=True))
            return low_back(low(matmul(hidden, out_matrix) + out_vector))
        expert_values = lax.map(jax.checkpoint(one_expert), (table, expert_up, expert_up_bias, expert_down, expert_down_bias))
        picked = expert_values.reshape(-1, D)[position]
        gate_values = jnp.take_along_axis(expert_probs, routes, axis=1)
        return after_attn + lax.optimization_barrier(jnp.sum(gate_values[:, :, None] * picked, axis=1))
    weights = tuple((member.astype(jnp.float32) for member in (dense_gains, dense_shifts, dense_qkv, dense_biases, dense_proj, dense_up, dense_up_bias, dense_down, moe_gains, moe_shifts, moe_qkv, moe_biases, moe_proj, router, expert_in, expert_in_bias, expert_out, expert_out_bias)))
    output, pullback = jax.vjp(forward, tokens.astype(jnp.float32), weights)
    token_grad, grads = pullback(cotangent.astype(jnp.float32))
    return (output.astype(jnp.bfloat16), token_grad, grads[0], grads[1], grads[2], grads[3], grads[4], grads[5], grads[6], grads[7], grads[8], grads[9], grads[10], grads[11], grads[12], grads[13], grads[14], grads[15], grads[16], grads[17])
```

```python
import functools

import jax
import jax.numpy as jnp
from jax import lax
from jax.experimental import pallas as pl
from jax.experimental.pallas import tpu as pltpu
from jax.sharding import PartitionSpec as P

HEADS = 8
SEQ = 197
EXTRA = 16
F32 = jnp.float32
BF16 = jnp.bfloat16
VMEM_LIMIT = 64000 * 1024


def round_up(value, step):
    return (value + step - 1) // step * step


def nn(left, right):
    return lax.dot_general(left, right, (((1,), (0,)), ((), ())), preferred_element_type=F32)


def nt(left, right):
    return lax.dot_general(left, right, (((1,), (1,)), ((), ())), preferred_element_type=F32)


def tn(left, right):
    return lax.dot_general(left, right, (((0,), (0,)), ((), ())), preferred_element_type=F32)


def split(value):
    high = value.astype(BF16)
    return high, (value - high.astype(F32)).astype(BF16)


def iota(shape, dim):
    return lax.broadcasted_iota(jnp.int32, shape, dim)


def aligned(index, step):
    return pl.ds(pl.multiple_of(index * step, step), step)


def normalised(values):
    average = jnp.mean(values, axis=-1, keepdims=True)
    centered = values - average
    variance = jnp.mean(centered * centered, axis=-1, keepdims=True)
    inverse = lax.rsqrt(variance + 1e-06)
    return centered * inverse, inverse


def norm_back(grad, gain, vhat, inverse):
    weighted = grad * gain
    first = jnp.mean(weighted, axis=-1, keepdims=True)
    second = jnp.mean(weighted * vhat, axis=-1, keepdims=True)
    return (weighted - first - vhat * second) * inverse


def gelu_pair(values):
    square = values * values
    inner = values * (0.7978845608 + (0.7978845608 * 0.044715) * square)
    tanh = jnp.tanh(inner)
    half = 0.5 * (1.0 + tanh)
    slope = 0.7978845608 + (3 * 0.7978845608 * 0.044715) * square
    return values * half, half + 0.5 * values * (1.0 - tanh * tanh) * slope


def half_masks(dtype):
    lane = iota((1, 128), 1)
    low = (lane < 64).astype(F32)
    return low.astype(dtype), (1.0 - low).astype(dtype)


def image_loop(images, body):
    def step(i, carry):
        body(i)
        return carry

    lax.fori_loop(0, images, step, 0)


def call(kernel, outs, scratch, flops, data_bytes, name):
    single = not isinstance(outs, (tuple, list))
    shapes = [outs] if single else list(outs)
    vmem = pl.BlockSpec(memory_space=pltpu.VMEM)
    smem = pl.BlockSpec(memory_space=pltpu.SMEM)

    def run(place, *args):
        return pl.pallas_call(
            kernel,
            out_shape=shapes[0] if single else shapes,
            in_specs=[smem] + [vmem] * len(args),
            out_specs=vmem if single else [vmem] * len(shapes),
            scratch_shapes=scratch,
            compiler_params=pltpu.CompilerParams(vmem_limit_bytes=VMEM_LIMIT),
            cost_estimate=pl.CostEstimate(
                flops=int(flops), bytes_accessed=int(data_bytes), transcendentals=0
            ),
            name=name,
        )(place, *args)

    return run


def attention_forward_part(images, padded, stream_of, gain, shift, qkv_w, biases, proj_w, norm_ref,
                           qkv_ref, prob_ref, mixed_ref, store):
    width = proj_w.shape[0]
    pairs = HEADS // 2

    def norm_step(i):
        rows = aligned(i, padded)
        vhat, _ = normalised(stream_of(rows))
        norm_ref[rows, :] = (vhat * gain + shift).astype(BF16)

    image_loop(images, norm_step)
    for n in range(6):
        cols = slice(n * 256, (n + 1) * 256)
        part = nn(norm_ref[...], qkv_w[:, cols])
        if n < 2:
            part = part + biases[0:1, cols]
        elif n >= 4:
            part = part + biases[1:2, (n - 4) * 256 : (n - 3) * 256]
        qkv_ref[:, cols] = part.astype(BF16)
    masks = half_masks(BF16)

    def heads_step(i):
        rows = aligned(i, padded)
        valid = iota((padded, padded), 1) < SEQ
        for j in range(pairs):
            cols = slice(j * 128, (j + 1) * 128)
            queries = qkv_ref[rows, cols]
            keys = qkv_ref[rows, width + j * 128 : width + (j + 1) * 128]
            values = qkv_ref[rows, 2 * width + j * 128 : 2 * width + (j + 1) * 128]
            total = None
            for h in range(2):
                scores = nt(queries * masks[h], keys) * 0.125
                scores = jnp.where(valid, scores, -1e30)
                shifted = jnp.exp(scores - jnp.max(scores, axis=-1, keepdims=True))
                weights = shifted / jnp.sum(shifted, axis=-1, keepdims=True)
                weights = weights.astype(BF16)
                prob_ref[i * HEADS + 2 * j + h] = weights
                part = nn(weights, values * masks[h])
                total = part if total is None else total + part
            mixed_ref[rows, cols] = total.astype(BF16)

    image_loop(images, heads_step)
    for n in range(width // 256):
        cols = slice(n * 256, (n + 1) * 256)
        store(cols, nn(mixed_ref[...], proj_w[:, cols]) + biases[2:3, cols])


def attention_backward_part(images, padded, upstream_ref, stream_of, gain, qkv_w, proj_w, norm_ref, qkv_ref,
                            prob_ref, mixed_ref, low_ref, mixed_grad_ref, joined_ref, proj_out,
                            qkv_out, wide_ref, finish):
    tokens, width = mixed_ref.shape
    pairs = HEADS // 2
    low_ref[...] = upstream_ref[...].astype(BF16)
    proj_bias = jnp.sum(low_ref[...].astype(F32), axis=0, keepdims=True)
    for n in range(width // 256):
        cols = slice(n * 256, (n + 1) * 256)
        proj_out[:, cols] = tn(mixed_ref[...], low_ref[:, cols]).astype(BF16)
        mixed_grad_ref[:, cols] = nt(low_ref[...], proj_w[cols, :]).astype(BF16)
    masks = half_masks(BF16)

    def heads_step(i):
        rows = aligned(i, padded)
        for j in range(pairs):
            cols = slice(j * 128, (j + 1) * 128)
            key_cols = slice(width + j * 128, width + (j + 1) * 128)
            value_cols = slice(2 * width + j * 128, 2 * width + (j + 1) * 128)
            queries = qkv_ref[rows, cols]
            keys = qkv_ref[rows, key_cols]
            values = qkv_ref[rows, value_cols]
            grads = mixed_grad_ref[rows, cols]
            query_grad = key_grad = value_grad = None
            for h in range(2):
                low = prob_ref[i * HEADS + 2 * j + h]
                weights = low.astype(F32)
                masked = grads * masks[h]
                weights_grad = nt(masked, values)
                center = jnp.sum(weights * weights_grad, axis=-1, keepdims=True)
                score_grad = (weights * (weights_grad - center)).astype(BF16)
                parts = (
                    nn(score_grad, keys * masks[h]),
                    tn(score_grad, queries * masks[h]),
                    tn(low, masked),
                )
                if query_grad is None:
                    query_grad, key_grad, value_grad = parts
                else:
                    query_grad, key_grad, value_grad = (
                        query_grad + parts[0], key_grad + parts[1], value_grad + parts[2])
            joined_ref[rows, cols] = (query_grad * 0.125).astype(BF16)
            joined_ref[rows, key_cols] = (key_grad * 0.125).astype(BF16)
            joined_ref[rows, value_cols] = value_grad.astype(BF16)

    image_loop(images, heads_step)
    for n in range(6):
        cols = slice(n * 256, (n + 1) * 256)
        qkv_out[:, cols] = tn(norm_ref[...], joined_ref[:, cols]).astype(BF16)
    for n in range(width // 256):
        cols = slice(n * 256, (n + 1) * 256)
        wide_ref[:, cols] = nt(joined_ref[...], qkv_w[cols, :])
    query_bias = jnp.sum(joined_ref[:, 0:width].astype(F32), axis=0, keepdims=True)
    value_bias = jnp.sum(joined_ref[:, 2 * width :].astype(F32), axis=0, keepdims=True)
    gain_grad, shift_grad = norm_back_part(
        images, padded, wide_ref, stream_of, gain, upstream_ref, finish)
    return gain_grad, shift_grad, query_bias, value_bias, proj_bias


def norm_back_part(images, padded, grad_ref, stream_of, gain, upstream_ref, finish):
    width = grad_ref.shape[1]

    def step(i, carry):
        gain_grad, shift_grad = carry
        rows = aligned(i, padded)
        vhat, inverse = normalised(stream_of(rows))
        grad = grad_ref[rows, :]
        finish(i, rows, upstream_ref[rows, :] + norm_back(grad, gain, vhat, inverse))
        return (
            gain_grad + jnp.sum(grad * vhat, axis=0, keepdims=True),
            shift_grad + jnp.sum(grad, axis=0, keepdims=True),
        )

    zero = jnp.zeros((1, width), F32)
    return lax.fori_loop(0, images, step, (zero, zero))


def write_shards(me, ways, keep_ref, send_ref, blocks, small):
    for r in range(ways):
        target = keep_ref if r % 2 == 0 else send_ref
        shard = lax.bitwise_xor(me, jnp.int32(r))
        at = 0
        for ref, lead in blocks:
            rows = ref.shape[-2] // ways
            window = pl.ds(pl.multiple_of(shard * rows, rows), rows)
            for n in range(ref.shape[-1] // 512):
                cols = slice(n * 512, (n + 1) * 512)
                value = ref[window, cols] if lead is None else ref[lead, window, cols]
                target[r // 2, at : at + rows, :] = value
                at += rows
        target[r // 2, at : at + small.shape[0], :] = small


def small_rows(rows, count):
    used = sum(row.shape[0] for row in rows)
    if used < count:
        rows = list(rows) + [jnp.zeros((count - used, rows[0].shape[1]), F32)]
    return jnp.concatenate(rows, axis=0).astype(BF16)


def rank_kernel(groups, local, slots, place, routes, routes_t, grads, rank_te, rank_et, *blocks):
    tokens, experts = rank_te.shape
    me = place[1]
    first = iota((tokens, tokens), 0)
    second = iota((tokens, tokens), 1)
    names = iota((tokens, experts), 1)
    chosen = (routes[:, 0:1] == names) | (routes[:, 1:2] == names)
    chosen = chosen.astype(F32)
    earlier = (second < first).astype(F32).astype(BF16)
    rank_te[...] = jnp.where(chosen > 0, nn(earlier, chosen.astype(BF16)), -1.0)
    names_t = iota((experts, tokens), 0)
    chosen_t = (routes_t[0:1, :] == names_t) | (routes_t[1:2, :] == names_t)
    chosen_t = chosen_t.astype(F32)
    later = (first < second).astype(F32).astype(BF16)
    rank_et[...] = jnp.where(chosen_t > 0, nn(chosen_t.astype(BF16), later), -1.0)
    low = grads[...].astype(BF16)
    slot = iota((slots, tokens), 0).astype(F32)
    for r in range(groups):
        for i in range(local):
            e = lax.bitwise_xor(me, jnp.int32(r)) * local + i
            pick = (rank_et[pl.ds(e, 1), :] == slot).astype(F32).astype(BF16)
            blocks[r][i * slots : (i + 1) * slots, :] = nn(pick, low).astype(BF16)


def forward_kernel(images, padded, groups, local, slots, place, tokens, gains, shifts, qkv_w, biases,
                   proj_w, up_w, up_bias, down_w, gains_two, shifts_two, qkv_two, biases_two, proj_two,
                   router, noise, rank_et,
                   norm_a, qkv_a, prob_a, mixed_a, middle, norm_m, hidden, slope, after_first,
                   norm_b, qkv_b, prob_b, mixed_b, after_attn, moe_norm, probs, *blocks):
    width = proj_w.shape[0]
    count = images * padded

    def store_middle(cols, branch):
        middle[:, cols] = tokens[:, cols].astype(F32) + branch

    attention_forward_part(images, padded, lambda rows: tokens[rows, :].astype(F32), gains[0:1, :],
                           shifts[0:1, :], qkv_w, biases, proj_w, norm_a, qkv_a, prob_a, mixed_a,
                           store_middle)

    def norm_step(i):
        rows = aligned(i, padded)
        vhat, _ = normalised(middle[rows, :])
        norm_m[rows, :] = (vhat * gains[1:2, :] + shifts[1:2, :]).astype(BF16)

    image_loop(images, norm_step)

    def up_step(n):
        cols = aligned(n, 256)
        pre = nn(norm_m[...], up_w[:, cols]) + up_bias[:, cols]
        value, gradient = gelu_pair(pre)
        hidden[:, cols] = value.astype(BF16)
        slope[:, cols] = gradient.astype(BF16)

    image_loop(up_w.shape[1] // 256, up_step)
    for n in range(width // 256):
        cols = slice(n * 256, (n + 1) * 256)
        after_first[:, cols] = middle[:, cols] + nn(hidden[...], down_w[:, cols]) + biases[3:4, cols]

    def store_after(cols, branch):
        after_attn[:, cols] = after_first[:, cols] + branch

    attention_forward_part(images, padded, lambda rows: after_first[rows, :], gains_two[0:1, :],
                           shifts_two[0:1, :], qkv_two, biases_two, proj_two, norm_b, qkv_b, prob_b,
                           mixed_b, store_after)

    def moe_step(i):
        rows = aligned(i, padded)
        vhat, _ = normalised(after_attn[rows, :])
        moe_norm[rows, :] = (vhat * gains_two[1:2, :] + shifts_two[1:2, :]).astype(BF16)

    image_loop(images, moe_step)
    logits = nn(moe_norm[...], router[...]) + noise[...]
    shifted = jnp.exp(logits - jnp.max(logits, axis=-1, keepdims=True))
    probabilities = shifted / jnp.sum(shifted, axis=-1, keepdims=True)
    probs[...] = probabilities
    high, low = split(probabilities)
    me = place[1]
    slot = iota((slots, count), 0).astype(F32)
    square = (iota((slots, slots), 0) == iota((slots, slots), 1)).astype(F32)
    lanes = iota((slots, router.shape[1]), 1)
    for r in range(groups):
        gates = []
        for i in range(local):
            e = lax.bitwise_xor(me, jnp.int32(r)) * local + i
            pick = (rank_et[pl.ds(e, 1), :] == slot).astype(F32).astype(BF16)
            blocks[r][i * slots : (i + 1) * slots, :] = nn(pick, moe_norm[...]).astype(BF16)
            both = nn(pick, high) + nn(pick, low)
            column = jnp.sum(jnp.where(lanes == e, both, 0.0), axis=1, keepdims=True)
            gates.append(jnp.sum(square * column, axis=0, keepdims=True))
        put_scalars(blocks[r], local * slots, gates, slots)


def put_scalars(ref, at, rows, slots):
    parts = []
    for row in rows:
        high, low = split(row)
        parts += [high.astype(F32), low.astype(F32)]
    parts.append(jnp.zeros((EXTRA - len(parts), slots), F32))
    ref[at : at + EXTRA, :] = jnp.zeros((EXTRA, ref.shape[1]), BF16)
    ref[at : at + EXTRA, 0:slots] = jnp.concatenate(parts, axis=0).astype(BF16)


def scalar_row(ref, at, i, slots):
    block = ref[at : at + EXTRA, 0:slots].astype(F32)
    return block[2 * i : 2 * i + 1, :] + block[2 * i + 1 : 2 * i + 2, :]


def early_kernel(groups, local, slots, place, out_w, *refs):
    blocks, product = refs[:groups], refs[groups]
    for i in range(local):
        for r in range(groups):
            rows = blocks[r][i * slots : (i + 1) * slots, :]
            for n in range(4):
                cols = slice(n * 512, (n + 1) * 512)
                product[i, r * slots : (r + 1) * slots, cols] = nt(rows, out_w[i, cols, :]).astype(BF16)


def expert_kernel(groups, local, slots, place, in_w, in_bias, out_bias, product, *refs):
    rows_in, grads_in = refs[:groups], refs[groups : 2 * groups]
    blocks, hidden, low = refs[2 * groups : 3 * groups], refs[3 * groups], refs[3 * groups + 1]
    joined = refs[3 * groups + 2]
    square = (iota((slots, slots), 0) == iota((slots, slots), 1)).astype(F32)
    scalars = [[] for _ in range(groups)]
    for i in range(local):
        for r in range(groups):
            joined[r * slots : (r + 1) * slots, :] = rows_in[r][i * slots : (i + 1) * slots, :]

        def up_step(n, total):
            cols = aligned(n, 256)
            pre = nn(joined[...], in_w[i, :, cols]) + in_bias[i : i + 1, cols]
            value, gradient = gelu_pair(pre)
            value = value.astype(BF16)
            hidden[i, :, cols] = value
            scale = product[i, :, cols].astype(F32)
            low[i, :, cols] = (scale * gradient).astype(BF16)
            both = value.astype(F32) * scale
            return total + both[:, 0:128] + both[:, 128:256]

        total = lax.fori_loop(0, in_w.shape[2] // 256, up_step, jnp.zeros((groups * slots, 128), F32))
        total = jnp.sum(total, axis=1, keepdims=True)
        for r in range(groups):
            g_rows = grads_in[r][i * slots : (i + 1) * slots, :].astype(F32)
            extra = jnp.sum(g_rows * out_bias[i : i + 1, :], axis=1, keepdims=True)
            column = total[r * slots : (r + 1) * slots, :] + extra
            scalars[r].append(jnp.sum(square * column, axis=0, keepdims=True))
        for n in range(2):
            cols = slice(n * 256, (n + 1) * 256)
            back = nt(low[i], in_w[i, cols, :]).astype(BF16)
            for r in range(groups):
                blocks[r][i * slots : (i + 1) * slots, cols] = back[r * slots : (r + 1) * slots, :]
    for r in range(groups):
        put_scalars(blocks[r], local * slots, scalars[r], slots)


def value_kernel(groups, local, slots, place, hidden, out_w, out_bias, *blocks):
    for i in range(local):
        for n in range(2):
            cols = slice(n * 256, (n + 1) * 256)
            value = nn(hidden[i], out_w[i, :, cols]) + out_bias[i : i + 1, cols]
            value = value.astype(BF16)
            for r in range(groups):
                blocks[r][i * slots : (i + 1) * slots, cols] = value[r * slots : (r + 1) * slots, :]


def weight_kernel(groups, local, slots, ways, place, hidden, low, *refs):
    rows_in, grads_in = refs[:groups], refs[groups : 2 * groups]
    keep, send = refs[2 * groups], refs[2 * groups + 1]
    scaled, value_grad, in_out, out_out = refs[2 * groups + 2 :]
    square = (iota((slots, slots), 0) == iota((slots, slots), 1)).astype(F32)
    small = []
    tail = []
    for i in range(local):
        gate_rows = []
        for r in range(groups):
            gate = scalar_row(rows_in[r], local * slots, i, slots)
            gate_rows.append(gate)
            column = jnp.sum(square * gate, axis=1, keepdims=True)
            own = slice(i * slots, (i + 1) * slots)
            at = slice(r * slots, (r + 1) * slots)
            scaled[at, :] = (rows_in[r][own, :].astype(F32) * column).astype(BF16)
            value_grad[at, :] = (grads_in[r][own, :].astype(F32) * column).astype(BF16)
        bias_parts = []
        for n in range(4):
            cols = slice(n * 512, (n + 1) * 512)
            in_out[i, :, cols] = tn(scaled[...], low[i, :, cols]).astype(BF16)
            total = jnp.zeros((8, 512), F32)
            for r in range(groups):
                high, rest = split(jnp.broadcast_to(gate_rows[r], (8, slots)))
                piece = low[i, r * slots : (r + 1) * slots, cols]
                total = total + nn(high, piece) + nn(rest, piece)
            bias_parts.append(total[0:1, :])
            out_out[i, cols, :] = tn(hidden[i, :, cols], value_grad[...]).astype(BF16)
        small += bias_parts
        tail.append(jnp.sum(value_grad[...].astype(F32), axis=0, keepdims=True))
    blocks = []
    for i in range(local):
        blocks += [(in_out, i), (out_out, i)]
    write_shards(place[0], ways, keep, send, blocks, small_rows(small + tail, 16))


def combine_columns(rank_te, probs, e, slots):
    tokens, experts = rank_te.shape
    mask = iota((tokens, experts), 1) == e
    column = jnp.sum(jnp.where(mask, rank_te[...], 0.0), axis=1, keepdims=True)
    gate = jnp.sum(jnp.where(mask, probs[...], 0.0), axis=1, keepdims=True)
    pick = (column == iota((tokens, slots), 1).astype(F32)).astype(F32)
    return mask, pick, gate


def output_kernel(groups, local, slots, place, rank_te, probs, after_attn, *refs):
    blocks, out, total = refs[:groups], refs[groups], refs[groups + 1]
    total[...] = after_attn[...]
    for r in range(groups):
        for i in range(local):
            e = lax.bitwise_xor(place[1], jnp.int32(r)) * local + i
            _, pick, gate = combine_columns(rank_te, probs, e, slots)
            total[...] += gate * nn(pick.astype(BF16), blocks[r][i * slots : (i + 1) * slots, :])
    out[...] = total[...].astype(BF16)


def attn_two_kernel(images, padded, groups, local, slots, ways, small_count, place, rank_te, probs,
                    after_attn, grads, gains, shifts, router, moe_norm, after_first, qkv_w, proj_w, norm_b,
                    qkv_b, prob_b, mixed_b, *refs):
    blocks = refs[:groups]
    stream_grad, keep, send = refs[groups : groups + 3]
    wide, upstream, low_ref, mixed_grad, joined, proj_out, qkv_out = refs[groups + 3 :]
    tokens, experts = rank_te.shape
    wide[...] = jnp.zeros_like(wide)
    gate_grad = jnp.zeros((tokens, experts), F32)
    for r in range(groups):
        for i in range(local):
            e = lax.bitwise_xor(place[1], jnp.int32(r)) * local + i
            mask, pick, gate = combine_columns(rank_te, probs, e, slots)
            scalars = scalar_row(blocks[r], local * slots, i, slots)
            column = jnp.sum(pick * scalars, axis=1, keepdims=True)
            gate_grad = jnp.where(mask, column, gate_grad)
            wide[...] += gate * nn(pick.astype(BF16), blocks[r][i * slots : (i + 1) * slots, :])
    probabilities = probs[...]
    inner = jnp.sum(probabilities * gate_grad, axis=1, keepdims=True)
    logit_grad = probabilities * (gate_grad - inner)
    high, rest = split(logit_grad)
    router_grad = tn(high, moe_norm[...]) + tn(rest, moe_norm[...])
    wide[...] += nt(high, router[...]) + nt(rest, router[...])

    def finish_moe(i, rows, value):
        upstream[rows, :] = value

    moe_gain, moe_shift = norm_back_part(images, padded, wide, lambda rows: after_attn[rows, :],
                                         gains[1:2, :], grads, finish_moe)

    def finish(i, rows, value):
        stream_grad[rows, :] = value

    sums = attention_backward_part(images, padded, upstream, lambda rows: after_first[rows, :],
                                   gains[0:1, :], qkv_w, proj_w, norm_b, qkv_b, prob_b, mixed_b, low_ref,
                                   mixed_grad, joined, proj_out, qkv_out, wide, finish)
    gain_grad, shift_grad, query_bias, value_bias, proj_bias = sums
    small = small_rows([gain_grad, moe_gain, shift_grad, moe_shift, query_bias, value_bias, proj_bias,
                        router_grad], small_count)
    write_shards(place[0], ways, keep, send, [(qkv_out, None), (proj_out, None)], small)


def mlp_back_kernel(images, padded, ways, place, upstream, middle, norm_m, hidden, slope, gains, up_w,
                    down_w, stream_grad, keep, send, low_ref, pre_grad, up_out, down_out, wide):
    width = up_w.shape[0]
    low_ref[...] = upstream[...].astype(BF16)
    down_bias = jnp.sum(low_ref[...].astype(F32), axis=0, keepdims=True)
    bias_parts = []
    for n in range(4):
        cols = slice(n * 512, (n + 1) * 512)
        hidden_grad = nt(low_ref[...], down_w[cols, :])
        value = (hidden_grad * slope[:, cols].astype(F32)).astype(BF16)
        pre_grad[:, cols] = value
        bias_parts.append(jnp.sum(value.astype(F32), axis=0, keepdims=True))
        down_out[cols, :] = tn(hidden[:, cols], low_ref[...]).astype(BF16)
        up_out[:, cols] = tn(norm_m[...], value).astype(BF16)
    for n in range(width // 256):
        cols = slice(n * 256, (n + 1) * 256)
        wide[:, cols] = nt(pre_grad[...], up_w[cols, :])

    def finish(i, rows, value):
        stream_grad[rows, :] = value

    gain_grad, shift_grad = norm_back_part(images, padded, wide, lambda rows: middle[rows, :],
                                           gains[1:2, :], upstream, finish)
    small = small_rows([gain_grad, shift_grad, down_bias] + bias_parts, 16)
    write_shards(place[0], ways, keep, send, [(up_out, None), (down_out, None)], small)


def attn_one_kernel(images, padded, ways, place, upstream, tokens, gains, qkv_w, proj_w, norm_a, qkv_a,
                    prob_a, mixed_a, stream_grad, keep, send, low_ref, mixed_grad, joined, proj_out,
                    qkv_out, wide):
    def finish(i, rows, value):
        stream_grad[rows, :] = value

    sums = attention_backward_part(images, padded, upstream, lambda rows: tokens[rows, :].astype(F32),
                                   gains[0:1, :], qkv_w, proj_w, norm_a, qkv_a, prob_a, mixed_a, low_ref,
                                   mixed_grad, joined, proj_out, qkv_out, wide, finish)
    write_shards(place[0], ways, keep, send, [(qkv_out, None), (proj_out, None)], small_rows(sums, 16))


def exchange(value, axis, mask):
    size = lax.axis_size(axis)
    return lax.ppermute(value, axis, [(i, i ^ mask) for i in range(size)])


def scatter_sum(keep, send, ways):
    arrived = exchange(send, "dp", 1)
    sums = [keep[j].astype(F32) + arrived[j].astype(F32) for j in range(ways // 2)]
    total = sums[0]
    parts = [exchange(sums[j].astype(BF16), "dp", 2 * j) for j in range(1, ways // 2)]
    for part in parts:
        total = total + part.astype(F32)
    return total


def group_sum(total):
    step = 1
    while step < lax.axis_size("expert"):
        low = total.astype(BF16)
        total = low.astype(F32) + exchange(low, "expert", step).astype(F32)
        step *= 2
    return total


def columns_of(rows, me, ways):
    share = rows.shape[1] // ways
    return lax.dynamic_slice_in_dim(rows, me * share, share, axis=1)


def joined_blocks(total, at, rows, count):
    parts = [total[at + n * rows : at + (n + 1) * rows, :] for n in range(count)]
    return jnp.concatenate(parts, axis=1), at + count * rows


def per_device(tokens, cotangent, dense_gains, dense_shifts, dense_qkv, dense_biases, dense_proj, dense_up,
               dense_up_bias, dense_down, moe_gains, moe_shifts, moe_qkv, moe_biases, moe_proj, router,
               router_noise, routes, expert_in, expert_in_bias, expert_out, expert_out_bias):
    count, width = tokens.shape
    top = routes.shape[1]
    experts = router.shape[1]
    groups = lax.axis_size("expert")
    ways = lax.axis_size("dp")
    local = expert_in.shape[0]
    ff = dense_up.shape[1]
    images = count // SEQ
    padded = round_up(SEQ, 16)
    full = images * padded
    capacity = max(2, (5 * count * top + 4 * experts - 1) // (4 * experts))
    slots = round_up(capacity, 16)
    me = lax.axis_index("dp").astype(jnp.int32)
    place = jnp.stack([me, lax.axis_index("expert").astype(jnp.int32)])

    def pad(array, value=0):
        shaped = array.reshape(images, SEQ, array.shape[1])
        shaped = jnp.pad(shaped, ((0, 0), (0, padded - SEQ), (0, 0)), constant_values=value)
        return shaped.reshape(full, array.shape[1])

    def unpad(array):
        return array.reshape(images, padded, width)[:, :SEQ, :].reshape(count, width)

    def shape(*dims, dtype=BF16):
        return jax.ShapeDtypeStruct(dims, dtype)

    tokens_p = pad(tokens)
    grads_p = pad(cotangent)
    noise_p = pad(router_noise)
    routes_p = pad(routes, -1)
    matmul = 2 * full * width

    row_block = local * slots
    ranks = call(
        functools.partial(rank_kernel, groups, local, slots),
        [shape(full, experts, dtype=F32), shape(experts, full, dtype=F32)]
        + [shape(row_block, width)] * groups,
        [], 2 * groups * row_block * full * width, 8e6, "ranks",
    )(place, routes_p, routes_p.T, grads_p)
    rank_te, rank_et, grad_blocks = ranks[0], ranks[1], ranks[2:]
    grad_blocks = [grad_blocks[0]] + [exchange(grad_blocks[r], "expert", r) for r in range(1, groups)]

    forward = call(
        functools.partial(forward_kernel, images, padded, groups, local, slots),
        [shape(full, width), shape(full, 3 * width), shape(images * HEADS, padded, padded),
         shape(full, width), shape(full, width, dtype=F32), shape(full, width), shape(full, ff),
         shape(full, ff), shape(full, width, dtype=F32), shape(full, width), shape(full, 3 * width),
         shape(images * HEADS, padded, padded), shape(full, width), shape(full, width, dtype=F32),
         shape(full, width), shape(full, experts, dtype=F32)]
        + [shape(row_block + EXTRA, width)] * groups,
        [], matmul * (8 * width + 2 * ff), 30e6, "forward",
    )(place, tokens_p, dense_gains, dense_shifts, dense_qkv, dense_biases, dense_proj, dense_up,
      dense_up_bias.reshape(1, ff), dense_down, moe_gains, moe_shifts, moe_qkv, moe_biases, moe_proj, router,
      noise_p, rank_et)
    (norm_a, qkv_a, prob_a, mixed_a, middle, norm_m, hidden, slope, after_first, norm_b, qkv_b, prob_b,
     mixed_b, after_attn, moe_norm, probs) = forward[:16]
    rows_out = forward[16:]
    row_blocks = [rows_out[0]] + [exchange(rows_out[r], "expert", r) for r in range(1, groups)]

    total_rows = groups * slots
    expert_flops = 2 * local * total_rows * width * ff
    product = call(
        functools.partial(early_kernel, groups, local, slots), shape(local, total_rows, ff), [],
        expert_flops, 12e6, "early",
    )(place, expert_out, *grad_blocks)
    expert = call(
        functools.partial(expert_kernel, groups, local, slots),
        [shape(row_block + EXTRA, width)] * groups
        + [shape(local, total_rows, ff), shape(local, total_rows, ff)],
        [pltpu.VMEM((total_rows, width), BF16)], 2 * expert_flops, 25e6, "experts",
    )(place, expert_in, expert_in_bias, expert_out_bias, product, *row_blocks, *grad_blocks)
    back_out, expert_hidden, expert_low = expert[:groups], expert[groups], expert[groups + 1]
    back_blocks = [back_out[0]] + [exchange(back_out[r], "expert", r) for r in range(1, groups)]

    value_out = call(
        functools.partial(value_kernel, groups, local, slots), [shape(row_block, width)] * groups, [],
        expert_flops, 12e6, "values",
    )(place, expert_hidden, expert_out, expert_out_bias)
    shard_rows = local * (width // ways * (ff // 512) + ff // ways) + 16
    keep, send = call(
        functools.partial(weight_kernel, groups, local, slots, ways),
        [shape(ways // 2, shard_rows, 512)] * 2,
        [pltpu.VMEM((total_rows, width), BF16), pltpu.VMEM((total_rows, width), BF16),
         pltpu.VMEM((local, width, ff), BF16), pltpu.VMEM((local, ff, width), BF16)],
        2 * expert_flops, 25e6, "weights",
    )(place, expert_hidden, expert_low, *row_blocks, *grad_blocks)
    tied = lax.optimization_barrier((tuple(value_out), tuple(back_blocks)))
    value_out, back_blocks = tied
    value_blocks = [value_out[0]] + [exchange(value_out[r], "expert", r) for r in range(1, groups)]
    expert_total = scatter_sum(keep, send, ways)

    attn_scratch = [pltpu.VMEM((full, width), BF16), pltpu.VMEM((full, width), BF16),
                    pltpu.VMEM((full, 3 * width), BF16), pltpu.VMEM((width, width), BF16),
                    pltpu.VMEM((width, 3 * width), BF16)]
    wide = pltpu.VMEM((full, width), F32)
    small_two = round_up(7 + experts, 16)
    attn_rows = width // ways * 4
    grad_first, keep, send = call(
        functools.partial(attn_two_kernel, images, padded, groups, local, slots, ways, small_two),
        [shape(full, width, dtype=F32)] + [shape(ways // 2, attn_rows + small_two, 512)] * 2,
        [wide, wide] + attn_scratch, matmul * 12 * width, 20e6, "attention_two",
    )(place, rank_te, probs, after_attn, grads_p, moe_gains, moe_shifts, router, moe_norm, after_first,
      moe_qkv, moe_proj, norm_b, qkv_b, prob_b, mixed_b, *back_blocks)
    two_total = group_sum(scatter_sum(keep, send, ways))

    grad_middle, keep, send = call(
        functools.partial(mlp_back_kernel, images, padded, ways),
        [shape(full, width, dtype=F32)]
        + [shape(ways // 2, width // ways * (ff // 512) + ff // ways + 16, 512)] * 2,
        [pltpu.VMEM((full, width), BF16), pltpu.VMEM((full, ff), BF16), pltpu.VMEM((width, ff), BF16),
         pltpu.VMEM((ff, width), BF16), wide],
        matmul * 4 * ff, 20e6, "mlp_back",
    )(place, grad_first, middle, norm_m, hidden, slope, dense_gains, dense_up, dense_down)
    mlp_total = group_sum(scatter_sum(keep, send, ways))

    token_grad, keep, send = call(
        functools.partial(attn_one_kernel, images, padded, ways),
        [shape(full, width, dtype=F32)] + [shape(ways // 2, attn_rows + 16, 512)] * 2,
        attn_scratch + [wide], matmul * 10 * width, 20e6, "attention_one",
    )(place, grad_middle, tokens_p, dense_gains, dense_qkv, dense_proj, norm_a, qkv_a, prob_a, mixed_a)
    one_total = group_sum(scatter_sum(keep, send, ways))

    out_tokens = call(
        functools.partial(output_kernel, groups, local, slots), shape(full, width),
        [wide], 2 * experts * slots * full * width, 5e6, "outputs",
    )(place, rank_te, probs, after_attn, *value_blocks)

    share = width // ways
    small = one_total[attn_rows:]
    dense_qkv_grad, at = joined_blocks(one_total, 0, share, 3)
    dense_proj_grad = one_total[at : at + share]
    mlp_small = mlp_total[share * (ff // 512) + ff // ways :]
    dense_up_grad, at = joined_blocks(mlp_total, 0, share, ff // 512)
    dense_down_grad = mlp_total[at : at + ff // ways]
    two_small = two_total[attn_rows:]
    moe_qkv_grad, at = joined_blocks(two_total, 0, share, 3)
    moe_proj_grad = two_total[at : at + share]
    gains_one = columns_of(jnp.stack([small[0], mlp_small[0]]), me, ways)
    shifts_one = columns_of(jnp.stack([small[1], mlp_small[1]]), me, ways)
    biases_one = columns_of(jnp.stack([small[2], small[3], small[4], mlp_small[2]]), me, ways)
    up_bias_grad = columns_of(mlp_small[3 : 3 + ff // 512].reshape(1, ff), me, ways).reshape(-1)
    two_cols = columns_of(two_small, me, ways)
    router_grad = two_cols[7 : 7 + experts].T
    in_grads, out_grads = [], []
    at = 0
    for i in range(local):
        part, at = joined_blocks(expert_total, at, share, ff // 512)
        in_grads.append(part)
        out_grads.append(expert_total[at : at + ff // ways])
        at += ff // ways
    expert_small = expert_total[at:]
    in_bias = columns_of(expert_small[0 : local * (ff // 512)].reshape(local, ff), me, ways)
    out_bias = columns_of(expert_small[local * (ff // 512) : local * (ff // 512) + local], me, ways)
    return (
        unpad(out_tokens), unpad(token_grad), gains_one, shifts_one, dense_qkv_grad, biases_one,
        dense_proj_grad, dense_up_grad, up_bias_grad, dense_down_grad, two_cols[0:2], two_cols[2:4],
        moe_qkv_grad, two_cols[4:7], moe_proj_grad, router_grad, jnp.stack(in_grads), in_bias,
        jnp.stack(out_grads), out_bias,
    )


def solution(mesh):
    rows = P(("dp", "expert"), None)
    placed = (rows, rows) + (P(),) * 14 + (
        rows, rows, P("expert", None, None), P("expert", None), P("expert", None, None), P("expert", None))
    col, row = P(None, "dp"), P("dp", None)
    return jax.shard_map(
        per_device,
        mesh=mesh,
        in_specs=placed,
        out_specs=(
            rows, rows, col, col, row, col, row, row, P("dp"), row, col, col, row, col, row, row,
            P("expert", "dp", None), P("expert", "dp"), P("expert", "dp", None), P("expert", "dp")),
        check_vma=False,
    )
```

```python
import functools

import jax
import jax.numpy as jnp
from jax import lax
from jax.experimental import pallas as pl
from jax.experimental.pallas import tpu as pltpu
from jax.sharding import PartitionSpec as P


HEADS = 8
SEQ = 197
EXTRA = 16
F32 = jnp.float32
BF16 = jnp.bfloat16
VMEM_LIMIT = 64000 * 1024


def round_up(value, step):
    return (value + step - 1) // step * step


def nn(left, right):
    return lax.dot_general(left, right, (((1,), (0,)), ((), ())), preferred_element_type=F32)


def nt(left, right):
    return lax.dot_general(left, right, (((1,), (1,)), ((), ())), preferred_element_type=F32)


def tn(left, right):
    return lax.dot_general(left, right, (((0,), (0,)), ((), ())), preferred_element_type=F32)


def split(value):
    high = value.astype(BF16)
    return high, (value - high.astype(F32)).astype(BF16)


def iota(shape, dim):
    return lax.broadcasted_iota(jnp.int32, shape, dim)


def aligned(index, step):
    return pl.ds(pl.multiple_of(index * step, step), step)


def normalised(values):
    average = jnp.mean(values, axis=-1, keepdims=True)
    centered = values - average
    variance = jnp.mean(centered * centered, axis=-1, keepdims=True)
    inverse = lax.rsqrt(variance + 1e-06)
    return centered * inverse, inverse


def norm_back(grad, gain, vhat, inverse):
    weighted = grad * gain
    first = jnp.mean(weighted, axis=-1, keepdims=True)
    second = jnp.mean(weighted * vhat, axis=-1, keepdims=True)
    return (weighted - first - vhat * second) * inverse


def gelu_pair(values):
    square = values * values
    inner = values * (0.7978845608 + (0.7978845608 * 0.044715) * square)
    tanh = jnp.tanh(inner)
    half = 0.5 * (1.0 + tanh)
    slope = 0.7978845608 + (3 * 0.7978845608 * 0.044715) * square
    return values * half, half + 0.5 * values * (1.0 - tanh * tanh) * slope


def half_masks(dtype):
    lane = iota((1, 128), 1)
    low = (lane < 64).astype(F32)
    return low.astype(dtype), (1.0 - low).astype(dtype)


def image_loop(images, body):
    def step(i, carry):
        body(i)
        return carry

    lax.fori_loop(0, images, step, 0)


def call(kernel, outs, scratch, flops, data_bytes):
    single = not isinstance(outs, (tuple, list))
    shapes = [outs] if single else list(outs)
    vmem = pl.BlockSpec(memory_space=pltpu.VMEM)
    smem = pl.BlockSpec(memory_space=pltpu.SMEM)

    def run(place, *args):
        return pl.pallas_call(
            kernel,
            out_shape=shapes[0] if single else shapes,
            in_specs=[smem] + [vmem] * len(args),
            out_specs=vmem if single else [vmem] * len(shapes),
            scratch_shapes=scratch,
            compiler_params=pltpu.CompilerParams(vmem_limit_bytes=VMEM_LIMIT),
            cost_estimate=pl.CostEstimate(
                flops=int(flops), bytes_accessed=int(data_bytes), transcendentals=0
            ),
        )(place, *args)

    return run


def attention_forward_part(images, padded, stream_of, gain, shift, qkv_w, biases, proj_w, norm_ref,
                           qkv_ref, prob_ref, mixed_ref, store):
    width = proj_w.shape[0]
    pairs = HEADS // 2

    def norm_step(i):
        rows = aligned(i, padded)
        vhat, _ = normalised(stream_of(rows))
        norm_ref[rows, :] = (vhat * gain + shift).astype(BF16)

    image_loop(images, norm_step)
    for n in range(6):
        cols = slice(n * 256, (n + 1) * 256)
        part = nn(norm_ref[...], qkv_w[:, cols])
        if n < 2:
            part = part + biases[0:1, cols]
        elif n >= 4:
            part = part + biases[1:2, (n - 4) * 256 : (n - 3) * 256]
        qkv_ref[:, cols] = part.astype(BF16)
    masks = half_masks(BF16)

    def heads_step(i):
        rows = aligned(i, padded)
        valid = iota((padded, padded), 1) < SEQ
        for j in range(pairs):
            cols = slice(j * 128, (j + 1) * 128)
            queries = qkv_ref[rows, cols]
            keys = qkv_ref[rows, width + j * 128 : width + (j + 1) * 128]
            values = qkv_ref[rows, 2 * width + j * 128 : 2 * width + (j + 1) * 128]
            total = None
            for h in range(2):
                scores = nt(queries * masks[h], keys) * 0.125
                scores = jnp.where(valid, scores, -1e30)
                shifted = jnp.exp(scores - jnp.max(scores, axis=-1, keepdims=True))
                weights = shifted / jnp.sum(shifted, axis=-1, keepdims=True)
                weights = weights.astype(BF16)
                prob_ref[i * HEADS + 2 * j + h] = weights
                part = nn(weights, values * masks[h])
                total = part if total is None else total + part
            mixed_ref[rows, cols] = total.astype(BF16)

    image_loop(images, heads_step)
    for n in range(width // 256):
        cols = slice(n * 256, (n + 1) * 256)
        store(cols, nn(mixed_ref[...], proj_w[:, cols]) + biases[2:3, cols])


def attention_backward_part(images, padded, upstream_ref, stream_of, gain, qkv_w, proj_w, norm_ref, qkv_ref,
                            prob_ref, mixed_ref, low_ref, mixed_grad_ref, joined_ref, proj_out,
                            qkv_out, wide_ref, finish):
    _, width = mixed_ref.shape
    pairs = HEADS // 2
    low_ref[...] = upstream_ref[...].astype(BF16)
    proj_bias = jnp.sum(low_ref[...].astype(F32), axis=0, keepdims=True)
    for n in range(width // 256):
        cols = slice(n * 256, (n + 1) * 256)
        proj_out[:, cols] = tn(mixed_ref[...], low_ref[:, cols]).astype(BF16)
        mixed_grad_ref[:, cols] = nt(low_ref[...], proj_w[cols, :]).astype(BF16)
    masks = half_masks(BF16)

    def heads_step(i):
        rows = aligned(i, padded)
        for j in range(pairs):
            cols = slice(j * 128, (j + 1) * 128)
            key_cols = slice(width + j * 128, width + (j + 1) * 128)
            value_cols = slice(2 * width + j * 128, 2 * width + (j + 1) * 128)
            queries = qkv_ref[rows, cols]
            keys = qkv_ref[rows, key_cols]
            values = qkv_ref[rows, value_cols]
            grads = mixed_grad_ref[rows, cols]
            query_grad = key_grad = value_grad = None
            for h in range(2):
                low = prob_ref[i * HEADS + 2 * j + h]
                weights = low.astype(F32)
                masked = grads * masks[h]
                weights_grad = nt(masked, values)
                center = jnp.sum(weights * weights_grad, axis=-1, keepdims=True)
                score_grad = (weights * (weights_grad - center)).astype(BF16)
                parts = (
                    nn(score_grad, keys * masks[h]),
                    tn(score_grad, queries * masks[h]),
                    tn(low, masked),
                )
                if query_grad is None:
                    query_grad, key_grad, value_grad = parts
                else:
                    query_grad, key_grad, value_grad = (
                        query_grad + parts[0], key_grad + parts[1], value_grad + parts[2])
            joined_ref[rows, cols] = (query_grad * 0.125).astype(BF16)
            joined_ref[rows, key_cols] = (key_grad * 0.125).astype(BF16)
            joined_ref[rows, value_cols] = value_grad.astype(BF16)

    image_loop(images, heads_step)
    for n in range(6):
        cols = slice(n * 256, (n + 1) * 256)
        qkv_out[:, cols] = tn(norm_ref[...], joined_ref[:, cols]).astype(BF16)
    for n in range(width // 256):
        cols = slice(n * 256, (n + 1) * 256)
        wide_ref[:, cols] = nt(joined_ref[...], qkv_w[cols, :])
    query_bias = jnp.sum(joined_ref[:, 0:width].astype(F32), axis=0, keepdims=True)
    value_bias = jnp.sum(joined_ref[:, 2 * width :].astype(F32), axis=0, keepdims=True)
    gain_grad, shift_grad = norm_back_part(
        images, padded, wide_ref, stream_of, gain, upstream_ref, finish)
    return gain_grad, shift_grad, query_bias, value_bias, proj_bias


def norm_back_part(images, padded, grad_ref, stream_of, gain, upstream_ref, finish):
    width = grad_ref.shape[1]

    def step(i, carry):
        gain_grad, shift_grad = carry
        rows = aligned(i, padded)
        vhat, inverse = normalised(stream_of(rows))
        grad = grad_ref[rows, :]
        finish(i, rows, upstream_ref[rows, :] + norm_back(grad, gain, vhat, inverse))
        return (
            gain_grad + jnp.sum(grad * vhat, axis=0, keepdims=True),
            shift_grad + jnp.sum(grad, axis=0, keepdims=True),
        )

    zero = jnp.zeros((1, width), F32)
    return lax.fori_loop(0, images, step, (zero, zero))


def write_shards(me, ways, keep_ref, send_ref, blocks, small):
    for r in range(ways):
        target = keep_ref if r % 2 == 0 else send_ref
        shard = lax.bitwise_xor(me, jnp.int32(r))
        at = 0
        for ref, lead in blocks:
            rows = ref.shape[-2] // ways
            window = pl.ds(pl.multiple_of(shard * rows, rows), rows)
            for n in range(ref.shape[-1] // 512):
                cols = slice(n * 512, (n + 1) * 512)
                value = ref[window, cols] if lead is None else ref[lead, window, cols]
                target[r // 2, at : at + rows, :] = value
                at += rows
        target[r // 2, at : at + small.shape[0], :] = small


def small_rows(rows, count):
    used = sum(row.shape[0] for row in rows)
    if used < count:
        rows = list(rows) + [jnp.zeros((count - used, rows[0].shape[1]), F32)]
    return jnp.concatenate(rows, axis=0).astype(BF16)


def rank_kernel(groups, local, slots, place, routes, routes_t, grads, rank_te, rank_et, *blocks):
    tokens, experts = rank_te.shape
    me = place[1]
    first = iota((tokens, tokens), 0)
    second = iota((tokens, tokens), 1)
    names = iota((tokens, experts), 1)
    chosen = (routes[:, 0:1] == names) | (routes[:, 1:2] == names)
    chosen = chosen.astype(F32)
    earlier = (second < first).astype(F32).astype(BF16)
    rank_te[...] = jnp.where(chosen > 0, nn(earlier, chosen.astype(BF16)), -1.0)
    names_t = iota((experts, tokens), 0)
    chosen_t = (routes_t[0:1, :] == names_t) | (routes_t[1:2, :] == names_t)
    chosen_t = chosen_t.astype(F32)
    later = (first < second).astype(F32).astype(BF16)
    rank_et[...] = jnp.where(chosen_t > 0, nn(chosen_t.astype(BF16), later), -1.0)
    low = grads[...].astype(BF16)
    slot = iota((slots, tokens), 0).astype(F32)
    for r in range(groups):
        for i in range(local):
            e = lax.bitwise_xor(me, jnp.int32(r)) * local + i
            pick = (rank_et[pl.ds(e, 1), :] == slot).astype(F32).astype(BF16)
            blocks[r][i * slots : (i + 1) * slots, :] = nn(pick, low).astype(BF16)


def forward_kernel(images, padded, groups, local, slots, place, tokens, gains, shifts, qkv_w, biases,
                   proj_w, up_w, up_bias, down_w, gains_two, shifts_two, qkv_two, biases_two, proj_two,
                   router, noise, rank_et,
                   norm_a, qkv_a, prob_a, mixed_a, middle, norm_m, hidden, slope, after_first,
                   norm_b, qkv_b, prob_b, mixed_b, after_attn, moe_norm, probs, *blocks):
    width = proj_w.shape[0]
    count = images * padded

    def store_middle(cols, branch):
        middle[:, cols] = tokens[:, cols].astype(F32) + branch

    attention_forward_part(images, padded, lambda rows: tokens[rows, :].astype(F32), gains[0:1, :],
                           shifts[0:1, :], qkv_w, biases, proj_w, norm_a, qkv_a, prob_a, mixed_a,
                           store_middle)

    def norm_step(i):
        rows = aligned(i, padded)
        vhat, _ = normalised(middle[rows, :])
        norm_m[rows, :] = (vhat * gains[1:2, :] + shifts[1:2, :]).astype(BF16)

    image_loop(images, norm_step)

    def up_step(n):
        cols = aligned(n, 256)
        pre = nn(norm_m[...], up_w[:, cols]) + up_bias[:, cols]
        value, gradient = gelu_pair(pre)
        hidden[:, cols] = value.astype(BF16)
        slope[:, cols] = gradient.astype(BF16)

    image_loop(up_w.shape[1] // 256, up_step)
    for n in range(width // 256):
        cols = slice(n * 256, (n + 1) * 256)
        after_first[:, cols] = middle[:, cols] + nn(hidden[...], down_w[:, cols]) + biases[3:4, cols]

    def store_after(cols, branch):
        after_attn[:, cols] = after_first[:, cols] + branch

    attention_forward_part(images, padded, lambda rows: after_first[rows, :], gains_two[0:1, :],
                           shifts_two[0:1, :], qkv_two, biases_two, proj_two, norm_b, qkv_b, prob_b,
                           mixed_b, store_after)

    def moe_step(i):
        rows = aligned(i, padded)
        vhat, _ = normalised(after_attn[rows, :])
        moe_norm[rows, :] = (vhat * gains_two[1:2, :] + shifts_two[1:2, :]).astype(BF16)

    image_loop(images, moe_step)
    logits = nn(moe_norm[...], router[...]) + noise[...]
    shifted = jnp.exp(logits - jnp.max(logits, axis=-1, keepdims=True))
    probabilities = shifted / jnp.sum(shifted, axis=-1, keepdims=True)
    probs[...] = probabilities
    high, low = split(probabilities)
    me = place[1]
    slot = iota((slots, count), 0).astype(F32)
    square = (iota((slots, slots), 0) == iota((slots, slots), 1)).astype(F32)
    lanes = iota((slots, router.shape[1]), 1)
    for r in range(groups):
        gates = []
        for i in range(local):
            e = lax.bitwise_xor(me, jnp.int32(r)) * local + i
            pick = (rank_et[pl.ds(e, 1), :] == slot).astype(F32).astype(BF16)
            blocks[r][i * slots : (i + 1) * slots, :] = nn(pick, moe_norm[...]).astype(BF16)
            both = nn(pick, high) + nn(pick, low)
            column = jnp.sum(jnp.where(lanes == e, both, 0.0), axis=1, keepdims=True)
            gates.append(jnp.sum(square * column, axis=0, keepdims=True))
        put_scalars(blocks[r], local * slots, gates, slots)


def put_scalars(ref, at, rows, slots):
    parts = []
    for row in rows:
        high, low = split(row)
        parts += [high.astype(F32), low.astype(F32)]
    parts.append(jnp.zeros((EXTRA - len(parts), slots), F32))
    ref[at : at + EXTRA, :] = jnp.zeros((EXTRA, ref.shape[1]), BF16)
    ref[at : at + EXTRA, 0:slots] = jnp.concatenate(parts, axis=0).astype(BF16)


def scalar_row(ref, at, i, slots):
    block = ref[at : at + EXTRA, 0:slots].astype(F32)
    return block[2 * i : 2 * i + 1, :] + block[2 * i + 1 : 2 * i + 2, :]


def early_kernel(groups, local, slots, place, out_w, *refs):
    blocks, product = refs[:groups], refs[groups]
    for i in range(local):
        for r in range(groups):
            rows = blocks[r][i * slots : (i + 1) * slots, :]
            for n in range(4):
                cols = slice(n * 512, (n + 1) * 512)
                product[i, r * slots : (r + 1) * slots, cols] = nt(rows, out_w[i, cols, :]).astype(BF16)


def expert_kernel(groups, local, slots, place, in_w, in_bias, out_bias, product, *refs):
    rows_in, grads_in = refs[:groups], refs[groups : 2 * groups]
    blocks, hidden, low = refs[2 * groups : 3 * groups], refs[3 * groups], refs[3 * groups + 1]
    joined = refs[3 * groups + 2]
    square = (iota((slots, slots), 0) == iota((slots, slots), 1)).astype(F32)
    scalars = [[] for _ in range(groups)]
    for i in range(local):
        for r in range(groups):
            joined[r * slots : (r + 1) * slots, :] = rows_in[r][i * slots : (i + 1) * slots, :]

        def up_step(n, total):
            cols = aligned(n, 256)
            pre = nn(joined[...], in_w[i, :, cols]) + in_bias[i : i + 1, cols]
            value, gradient = gelu_pair(pre)
            value = value.astype(BF16)
            hidden[i, :, cols] = value
            scale = product[i, :, cols].astype(F32)
            low[i, :, cols] = (scale * gradient).astype(BF16)
            both = value.astype(F32) * scale
            return total + both[:, 0:128] + both[:, 128:256]

        total = lax.fori_loop(0, in_w.shape[2] // 256, up_step, jnp.zeros((groups * slots, 128), F32))
        total = jnp.sum(total, axis=1, keepdims=True)
        for r in range(groups):
            g_rows = grads_in[r][i * slots : (i + 1) * slots, :].astype(F32)
            extra = jnp.sum(g_rows * out_bias[i : i + 1, :], axis=1, keepdims=True)
            column = total[r * slots : (r + 1) * slots, :] + extra
            scalars[r].append(jnp.sum(square * column, axis=0, keepdims=True))
        for n in range(2):
            cols = slice(n * 256, (n + 1) * 256)
            back = nt(low[i], in_w[i, cols, :]).astype(BF16)
            for r in range(groups):
                blocks[r][i * slots : (i + 1) * slots, cols] = back[r * slots : (r + 1) * slots, :]
    for r in range(groups):
        put_scalars(blocks[r], local * slots, scalars[r], slots)


def value_kernel(groups, local, slots, place, hidden, out_w, out_bias, *blocks):
    for i in range(local):
        for n in range(2):
            cols = slice(n * 256, (n + 1) * 256)
            value = nn(hidden[i], out_w[i, :, cols]) + out_bias[i : i + 1, cols]
            value = value.astype(BF16)
            for r in range(groups):
                blocks[r][i * slots : (i + 1) * slots, cols] = value[r * slots : (r + 1) * slots, :]


def weight_kernel(groups, local, slots, ways, place, hidden, low, *refs):
    rows_in, grads_in = refs[:groups], refs[groups : 2 * groups]
    keep, send = refs[2 * groups], refs[2 * groups + 1]
    scaled, value_grad, in_out, out_out = refs[2 * groups + 2 :]
    square = (iota((slots, slots), 0) == iota((slots, slots), 1)).astype(F32)
    small = []
    tail = []
    for i in range(local):
        gate_rows = []
        for r in range(groups):
            gate = scalar_row(rows_in[r], local * slots, i, slots)
            gate_rows.append(gate)
            column = jnp.sum(square * gate, axis=1, keepdims=True)
            own = slice(i * slots, (i + 1) * slots)
            at = slice(r * slots, (r + 1) * slots)
            scaled[at, :] = (rows_in[r][own, :].astype(F32) * column).astype(BF16)
            value_grad[at, :] = (grads_in[r][own, :].astype(F32) * column).astype(BF16)
        bias_parts = []
        for n in range(4):
            cols = slice(n * 512, (n + 1) * 512)
            in_out[i, :, cols] = tn(scaled[...], low[i, :, cols]).astype(BF16)
            total = jnp.zeros((8, 512), F32)
            for r in range(groups):
                high, rest = split(jnp.broadcast_to(gate_rows[r], (8, slots)))
                piece = low[i, r * slots : (r + 1) * slots, cols]
                total = total + nn(high, piece) + nn(rest, piece)
            bias_parts.append(total[0:1, :])
            out_out[i, cols, :] = tn(hidden[i, :, cols], value_grad[...]).astype(BF16)
        small += bias_parts
        tail.append(jnp.sum(value_grad[...].astype(F32), axis=0, keepdims=True))
    blocks = []
    for i in range(local):
        blocks += [(in_out, i), (out_out, i)]
    write_shards(place[0], ways, keep, send, blocks, small_rows(small + tail, 16))


def combine_columns(rank_te, probs, e, slots):
    tokens, experts = rank_te.shape
    mask = iota((tokens, experts), 1) == e
    column = jnp.sum(jnp.where(mask, rank_te[...], 0.0), axis=1, keepdims=True)
    gate = jnp.sum(jnp.where(mask, probs[...], 0.0), axis=1, keepdims=True)
    pick = (column == iota((tokens, slots), 1).astype(F32)).astype(F32)
    return mask, pick, gate


def output_kernel(groups, local, slots, place, rank_te, probs, after_attn, *refs):
    blocks, out, total = refs[:groups], refs[groups], refs[groups + 1]
    total[...] = after_attn[...]
    for r in range(groups):
        for i in range(local):
            e = lax.bitwise_xor(place[1], jnp.int32(r)) * local + i
            _, pick, gate = combine_columns(rank_te, probs, e, slots)
            total[...] += gate * nn(pick.astype(BF16), blocks[r][i * slots : (i + 1) * slots, :])
    out[...] = total[...].astype(BF16)


def attn_two_kernel(images, padded, groups, local, slots, ways, small_count, place, rank_te, probs,
                    after_attn, grads, gains, shifts, router, moe_norm, after_first, qkv_w, proj_w, norm_b,
                    qkv_b, prob_b, mixed_b, *refs):
    blocks = refs[:groups]
    stream_grad, keep, send = refs[groups : groups + 3]
    wide, upstream, low_ref, mixed_grad, joined, proj_out, qkv_out = refs[groups + 3 :]
    tokens, experts = rank_te.shape
    wide[...] = jnp.zeros_like(wide)
    gate_grad = jnp.zeros((tokens, experts), F32)
    for r in range(groups):
        for i in range(local):
            e = lax.bitwise_xor(place[1], jnp.int32(r)) * local + i
            mask, pick, gate = combine_columns(rank_te, probs, e, slots)
            scalars = scalar_row(blocks[r], local * slots, i, slots)
            column = jnp.sum(pick * scalars, axis=1, keepdims=True)
            gate_grad = jnp.where(mask, column, gate_grad)
            wide[...] += gate * nn(pick.astype(BF16), blocks[r][i * slots : (i + 1) * slots, :])
    probabilities = probs[...]
    inner = jnp.sum(probabilities * gate_grad, axis=1, keepdims=True)
    logit_grad = probabilities * (gate_grad - inner)
    high, rest = split(logit_grad)
    router_grad = tn(high, moe_norm[...]) + tn(rest, moe_norm[...])
    wide[...] += nt(high, router[...]) + nt(rest, router[...])

    def finish_moe(i, rows, value):
        upstream[rows, :] = value

    moe_gain, moe_shift = norm_back_part(images, padded, wide, lambda rows: after_attn[rows, :],
                                         gains[1:2, :], grads, finish_moe)

    def finish(i, rows, value):
        stream_grad[rows, :] = value

    sums = attention_backward_part(images, padded, upstream, lambda rows: after_first[rows, :],
                                   gains[0:1, :], qkv_w, proj_w, norm_b, qkv_b, prob_b, mixed_b, low_ref,
                                   mixed_grad, joined, proj_out, qkv_out, wide, finish)
    gain_grad, shift_grad, query_bias, value_bias, proj_bias = sums
    small = small_rows([gain_grad, moe_gain, shift_grad, moe_shift, query_bias, value_bias, proj_bias,
                        router_grad], small_count)
    write_shards(place[0], ways, keep, send, [(qkv_out, None), (proj_out, None)], small)


def mlp_back_kernel(images, padded, ways, place, upstream, middle, norm_m, hidden, slope, gains, up_w,
                    down_w, stream_grad, keep, send, low_ref, pre_grad, up_out, down_out, wide):
    width = up_w.shape[0]
    low_ref[...] = upstream[...].astype(BF16)
    down_bias = jnp.sum(low_ref[...].astype(F32), axis=0, keepdims=True)
    bias_parts = []
    for n in range(4):
        cols = slice(n * 512, (n + 1) * 512)
        hidden_grad = nt(low_ref[...], down_w[cols, :])
        value = (hidden_grad * slope[:, cols].astype(F32)).astype(BF16)
        pre_grad[:, cols] = value
        bias_parts.append(jnp.sum(value.astype(F32), axis=0, keepdims=True))
        down_out[cols, :] = tn(hidden[:, cols], low_ref[...]).astype(BF16)
        up_out[:, cols] = tn(norm_m[...], value).astype(BF16)
    for n in range(width // 256):
        cols = slice(n * 256, (n + 1) * 256)
        wide[:, cols] = nt(pre_grad[...], up_w[cols, :])

    def finish(i, rows, value):
        stream_grad[rows, :] = value

    gain_grad, shift_grad = norm_back_part(images, padded, wide, lambda rows: middle[rows, :],
                                           gains[1:2, :], upstream, finish)
    small = small_rows([gain_grad, shift_grad, down_bias] + bias_parts, 16)
    write_shards(place[0], ways, keep, send, [(up_out, None), (down_out, None)], small)


def attn_one_kernel(images, padded, ways, place, upstream, tokens, gains, qkv_w, proj_w, norm_a, qkv_a,
                    prob_a, mixed_a, stream_grad, keep, send, low_ref, mixed_grad, joined, proj_out,
                    qkv_out, wide):
    def finish(i, rows, value):
        stream_grad[rows, :] = value

    sums = attention_backward_part(images, padded, upstream, lambda rows: tokens[rows, :].astype(F32),
                                   gains[0:1, :], qkv_w, proj_w, norm_a, qkv_a, prob_a, mixed_a, low_ref,
                                   mixed_grad, joined, proj_out, qkv_out, wide, finish)
    write_shards(place[0], ways, keep, send, [(qkv_out, None), (proj_out, None)], small_rows(sums, 16))


def exchange(value, axis, mask):
    size = lax.axis_size(axis)
    return lax.ppermute(value, axis, [(i, i ^ mask) for i in range(size)])


def spread(blocks):
    return [blocks[0]] + [exchange(blocks[r], "expert", r) for r in range(1, len(blocks))]


def core_sum(keep, send, ways):
    arrived = exchange(send, "dp", 1)
    sums = [keep[j].astype(F32) + arrived[j].astype(F32) for j in range(ways // 2)]
    return (sums[0],) + tuple(value.astype(BF16) for value in sums[1:])


def plane_start(sums, ways):
    return tuple(exchange(sums[j], "dp", 2 * j) for j in range(1, ways // 2))


def plane_sum(sums, parts):
    total = sums[0]
    for part in parts:
        total = total + part.astype(F32)
    return total


def group_sum(total):
    step = 1
    while step < lax.axis_size("expert"):
        low = total.astype(BF16)
        total = low.astype(F32) + exchange(low, "expert", step).astype(F32)
        step *= 2
    return total


def columns_of(rows, me, ways):
    share = rows.shape[1] // ways
    return lax.dynamic_slice_in_dim(rows, me * share, share, axis=1)


def joined_blocks(total, at, rows, count):
    parts = [total[at + n * rows : at + (n + 1) * rows, :] for n in range(count)]
    return jnp.concatenate(parts, axis=1), at + count * rows


def per_device(tokens, cotangent, dense_gains, dense_shifts, dense_qkv, dense_biases, dense_proj, dense_up,
               dense_up_bias, dense_down, moe_gains, moe_shifts, moe_qkv, moe_biases, moe_proj, router,
               router_noise, routes, expert_in, expert_in_bias, expert_out, expert_out_bias):
    count, width = tokens.shape
    top = routes.shape[1]
    experts = router.shape[1]
    groups = lax.axis_size("expert")
    ways = lax.axis_size("dp")
    local = expert_in.shape[0]
    ff = dense_up.shape[1]
    images = count // SEQ
    padded = round_up(SEQ, 16)
    full = images * padded
    capacity = max(2, (5 * count * top + 4 * experts - 1) // (4 * experts))
    slots = round_up(capacity, 16)
    me = lax.axis_index("dp").astype(jnp.int32)
    place = jnp.stack([me, lax.axis_index("expert").astype(jnp.int32)])

    def pad(array, value=0):
        shaped = array.reshape(images, SEQ, array.shape[1])
        shaped = jnp.pad(shaped, ((0, 0), (0, padded - SEQ), (0, 0)), constant_values=value)
        return shaped.reshape(full, array.shape[1])

    def unpad(array):
        return array.reshape(images, padded, width)[:, :SEQ, :].reshape(count, width)

    def shape(*dims, dtype=BF16):
        return jax.ShapeDtypeStruct(dims, dtype)

    tokens_p = pad(tokens)
    grads_p = pad(cotangent)
    noise_p = pad(router_noise)
    routes_p = pad(routes, -1)
    matmul = 2 * full * width

    row_block = local * slots
    ranks = call(
        functools.partial(rank_kernel, groups, local, slots),
        [shape(full, experts, dtype=F32), shape(experts, full, dtype=F32)]
        + [shape(row_block, width)] * groups,
        [], 2 * groups * row_block * full * width, 8e6,
    )(place, routes_p, routes_p.T, grads_p)
    rank_te, rank_et, grad_blocks = ranks[0], ranks[1], ranks[2:]
    grad_blocks = spread(grad_blocks)

    forward = call(
        functools.partial(forward_kernel, images, padded, groups, local, slots),
        [shape(full, width), shape(full, 3 * width), shape(images * HEADS, padded, padded),
         shape(full, width), shape(full, width, dtype=F32), shape(full, width), shape(full, ff),
         shape(full, ff), shape(full, width, dtype=F32), shape(full, width), shape(full, 3 * width),
         shape(images * HEADS, padded, padded), shape(full, width), shape(full, width, dtype=F32),
         shape(full, width), shape(full, experts, dtype=F32)]
        + [shape(row_block + EXTRA, width)] * groups,
        [], matmul * (8 * width + 2 * ff), 30e6,
    )(place, tokens_p, dense_gains, dense_shifts, dense_qkv, dense_biases, dense_proj, dense_up,
      dense_up_bias.reshape(1, ff), dense_down, moe_gains, moe_shifts, moe_qkv, moe_biases, moe_proj, router,
      noise_p, rank_et)
    (norm_a, qkv_a, prob_a, mixed_a, middle, norm_m, hidden, slope, after_first, norm_b, qkv_b, prob_b,
     mixed_b, after_attn, moe_norm, probs) = forward[:16]
    rows_out = forward[16:]
    row_blocks = spread(rows_out)

    total_rows = groups * slots
    expert_flops = 2 * local * total_rows * width * ff
    product = call(
        functools.partial(early_kernel, groups, local, slots), shape(local, total_rows, ff), [],
        expert_flops, 12e6,
    )(place, expert_out, *grad_blocks)
    expert = call(
        functools.partial(expert_kernel, groups, local, slots),
        [shape(row_block + EXTRA, width)] * groups
        + [shape(local, total_rows, ff), shape(local, total_rows, ff)],
        [pltpu.VMEM((total_rows, width), BF16)], 2 * expert_flops, 25e6,
    )(place, expert_in, expert_in_bias, expert_out_bias, product, *row_blocks, *grad_blocks)
    back_out, expert_hidden, expert_low = expert[:groups], expert[groups], expert[groups + 1]
    back_blocks = spread(back_out)

    shard_rows = local * (width // ways * (ff // 512) + ff // ways) + 16
    keep, send = call(
        functools.partial(weight_kernel, groups, local, slots, ways),
        [shape(ways // 2, shard_rows, 512)] * 2,
        [pltpu.VMEM((total_rows, width), BF16), pltpu.VMEM((total_rows, width), BF16),
         pltpu.VMEM((local, width, ff), BF16), pltpu.VMEM((local, ff, width), BF16)],
        2 * expert_flops, 25e6,
    )(place, expert_hidden, expert_low, *row_blocks, *grad_blocks)
    expert_hidden, keep, send = lax.optimization_barrier((expert_hidden, keep, send))
    value_out = call(
        functools.partial(value_kernel, groups, local, slots), [shape(row_block, width)] * groups, [],
        expert_flops, 12e6,
    )(place, expert_hidden, expert_out, expert_out_bias)
    expert_sums = core_sum(keep, send, ways)
    value_out, back_blocks, expert_sums, rank_te = lax.optimization_barrier(
        (tuple(value_out), tuple(back_blocks), expert_sums, rank_te))
    value_blocks = spread(value_out)
    expert_parts = plane_start(expert_sums, ways)

    attn_scratch = [pltpu.VMEM((full, width), BF16), pltpu.VMEM((full, width), BF16),
                    pltpu.VMEM((full, 3 * width), BF16), pltpu.VMEM((width, width), BF16),
                    pltpu.VMEM((width, 3 * width), BF16)]
    wide = pltpu.VMEM((full, width), F32)
    small_two = round_up(7 + experts, 16)
    attn_rows = width // ways * 4
    grad_first, keep, send = call(
        functools.partial(attn_two_kernel, images, padded, groups, local, slots, ways, small_two),
        [shape(full, width, dtype=F32)] + [shape(ways // 2, attn_rows + small_two, 512)] * 2,
        [wide, wide] + attn_scratch, matmul * 12 * width, 20e6,
    )(place, rank_te, probs, after_attn, grads_p, moe_gains, moe_shifts, router, moe_norm, after_first,
      moe_qkv, moe_proj, norm_b, qkv_b, prob_b, mixed_b, *back_blocks)
    two_sums = core_sum(keep, send, ways)

    grad_middle, keep, send = call(
        functools.partial(mlp_back_kernel, images, padded, ways),
        [shape(full, width, dtype=F32)]
        + [shape(ways // 2, width // ways * (ff // 512) + ff // ways + 16, 512)] * 2,
        [pltpu.VMEM((full, width), BF16), pltpu.VMEM((full, ff), BF16), pltpu.VMEM((width, ff), BF16),
         pltpu.VMEM((ff, width), BF16), wide],
        matmul * 4 * ff, 20e6,
    )(place, grad_first, middle, norm_m, hidden, slope, dense_gains, dense_up, dense_down)
    grad_middle, two_sums = lax.optimization_barrier((grad_middle, two_sums))
    two_parts = plane_start(two_sums, ways)
    mlp_sums = core_sum(keep, send, ways)

    token_grad, keep, send = call(
        functools.partial(attn_one_kernel, images, padded, ways),
        [shape(full, width, dtype=F32)] + [shape(ways // 2, attn_rows + 16, 512)] * 2,
        attn_scratch + [wide], matmul * 10 * width, 20e6,
    )(place, grad_middle, tokens_p, dense_gains, dense_qkv, dense_proj, norm_a, qkv_a, prob_a, mixed_a)
    token_grad, keep, send, mlp_sums, expert_parts, two_parts = lax.optimization_barrier(
        (token_grad, keep, send, mlp_sums, expert_parts, two_parts))
    one_sums = core_sum(keep, send, ways)
    mlp_parts = plane_start(mlp_sums, ways)
    one_parts = plane_start(one_sums, ways)
    expert_total = plane_sum(expert_sums, expert_parts)
    two_total = group_sum(plane_sum(two_sums, two_parts))
    mlp_total = group_sum(plane_sum(mlp_sums, mlp_parts))
    one_total = group_sum(plane_sum(one_sums, one_parts))

    out_tokens = call(
        functools.partial(output_kernel, groups, local, slots), shape(full, width),
        [wide], 2 * experts * slots * full * width, 5e6,
    )(place, rank_te, probs, after_attn, *value_blocks)

    share = width // ways
    small = one_total[attn_rows:]
    dense_qkv_grad, at = joined_blocks(one_total, 0, share, 3)
    dense_proj_grad = one_total[at : at + share]
    mlp_small = mlp_total[share * (ff // 512) + ff // ways :]
    dense_up_grad, at = joined_blocks(mlp_total, 0, share, ff // 512)
    dense_down_grad = mlp_total[at : at + ff // ways]
    two_small = two_total[attn_rows:]
    moe_qkv_grad, at = joined_blocks(two_total, 0, share, 3)
    moe_proj_grad = two_total[at : at + share]
    gains_one = columns_of(jnp.stack([small[0], mlp_small[0]]), me, ways)
    shifts_one = columns_of(jnp.stack([small[1], mlp_small[1]]), me, ways)
    biases_one = columns_of(jnp.stack([small[2], small[3], small[4], mlp_small[2]]), me, ways)
    up_bias_grad = columns_of(mlp_small[3 : 3 + ff // 512].reshape(1, ff), me, ways).reshape(-1)
    two_cols = columns_of(two_small, me, ways)
    router_grad = two_cols[7 : 7 + experts].T
    in_grads, out_grads = [], []
    at = 0
    for _ in range(local):
        part, at = joined_blocks(expert_total, at, share, ff // 512)
        in_grads.append(part)
        out_grads.append(expert_total[at : at + ff // ways])
        at += ff // ways
    expert_small = expert_total[at:]
    in_bias = columns_of(expert_small[0 : local * (ff // 512)].reshape(local, ff), me, ways)
    out_bias = columns_of(expert_small[local * (ff // 512) : local * (ff // 512) + local], me, ways)
    return (
        unpad(out_tokens), unpad(token_grad), gains_one, shifts_one, dense_qkv_grad, biases_one,
        dense_proj_grad, dense_up_grad, up_bias_grad, dense_down_grad, two_cols[0:2], two_cols[2:4],
        moe_qkv_grad, two_cols[4:7], moe_proj_grad, router_grad, jnp.stack(in_grads), in_bias,
        jnp.stack(out_grads), out_bias,
    )


def solution(mesh):
    rows = P(("dp", "expert"), None)
    placed = (rows, rows) + (P(),) * 14 + (
        rows, rows, P("expert", None, None), P("expert", None), P("expert", None, None), P("expert", None))
    col, row = P(None, "dp"), P("dp", None)
    return jax.shard_map(
        per_device,
        mesh=mesh,
        in_specs=placed,
        out_specs=(
            rows, rows, col, col, row, col, row, row, P("dp"), row, col, col, row, col, row, row,
            P("expert", "dp", None), P("expert", "dp"), P("expert", "dp", None), P("expert", "dp")),
        check_vma=False,
    )
```

```python
import functools

import jax
import jax.numpy as jnp
from jax import lax
from jax.experimental import pallas as pl
from jax.experimental.pallas import tpu as pltpu
from jax.sharding import PartitionSpec as P


HEADS = 8
SEQ = 197
EXTRA = 16
F32 = jnp.float32
BF16 = jnp.bfloat16


def round_up(value, step):
    return (value + step - 1) // step * step


def nn(left, right):
    return lax.dot_general(left, right, (((1,), (0,)), ((), ())), preferred_element_type=F32)


def nt(left, right):
    return lax.dot_general(left, right, (((1,), (1,)), ((), ())), preferred_element_type=F32)


def tn(left, right):
    return lax.dot_general(left, right, (((0,), (0,)), ((), ())), preferred_element_type=F32)


def split(value):
    high = value.astype(BF16)
    return high, (value - high.astype(F32)).astype(BF16)


def iota(shape, dim):
    return lax.broadcasted_iota(jnp.int32, shape, dim)


def aligned(index, step):
    return pl.ds(pl.multiple_of(index * step, step), step)


def normalised(values):
    average = jnp.mean(values, axis=-1, keepdims=True)
    centered = values - average
    variance = jnp.mean(centered * centered, axis=-1, keepdims=True)
    inverse = lax.rsqrt(variance + 1e-06)
    return centered * inverse, inverse


def norm_back(grad, gain, vhat, inverse):
    weighted = grad * gain
    first = jnp.mean(weighted, axis=-1, keepdims=True)
    second = jnp.mean(weighted * vhat, axis=-1, keepdims=True)
    return (weighted - first - vhat * second) * inverse


def gelu_pair(values):
    square = values * values
    inner = values * (0.7978845608 + (0.7978845608 * 0.044715) * square)
    tanh = jnp.tanh(inner)
    half = 0.5 * (1.0 + tanh)
    slope = 0.7978845608 + (3 * 0.7978845608 * 0.044715) * square
    return values * half, half + 0.5 * values * (1.0 - tanh * tanh) * slope


def half_masks(dtype):
    lane = iota((1, 128), 1)
    low = (lane < 64).astype(F32)
    return low.astype(dtype), (1.0 - low).astype(dtype)


def image_loop(images, body):
    def step(i, carry):
        body(i)
        return carry

    lax.fori_loop(0, images, step, 0)


class Staged:
    def __init__(self, hbm, vmem, sems, base, parts, incoming):
        self.vmem = vmem
        self.waited = set()
        self.copies = []
        for i in range(parts):
            far, near = (hbm, vmem) if parts == 1 else (hbm.at[i], vmem.at[i])
            pair = (far, near) if incoming else (near, far)
            self.copies.append(pltpu.make_async_copy(*pair, sems.at[base + i]))

    def start(self, part=None):
        for i, copy in enumerate(self.copies):
            if part is None or part == i:
                copy.start()

    def get(self, part=None):
        for i, copy in enumerate(self.copies):
            if (part is None or part == i) and i not in self.waited:
                self.waited.add(i)
                copy.wait()
        return self.vmem


class Hbm:
    def __init__(self, value, parts=1):
        self.value, self.parts = value, parts


def call(kernel, outs, scratch, flops, data_bytes, limit):
    vmem = pl.BlockSpec(memory_space=pltpu.VMEM)
    smem = pl.BlockSpec(memory_space=pltpu.SMEM)
    hbm = pl.BlockSpec(memory_space=pltpu.HBM)

    def run(place, *args):
        operands = list(args) + list(outs)
        staged = [one if isinstance(one, Hbm) else None for one in operands]
        values = [one.value if isinstance(one, Hbm) else one for one in operands]
        buffers = [pltpu.VMEM(values[i].shape, values[i].dtype) for i, one in enumerate(staged) if one]
        slots = sum(one.parts for one in staged if one)

        def body(place_ref, *refs):
            refs = list(refs)
            main, rest = refs[: len(operands)], refs[len(operands) :]
            own, copies, sems = rest[: len(scratch)], rest[len(scratch) : -1], rest[-1]
            base, at, wrapped = 0, 0, []
            for i, one in enumerate(staged):
                if one is None:
                    wrapped.append(main[i])
                    continue
                wrapped.append(Staged(main[i], copies[at], sems, base, one.parts, i < len(args)))
                base += one.parts
                at += 1
            for i, one in enumerate(wrapped[: len(args)]):
                if staged[i]:
                    one.start()
            kernel(place_ref, *wrapped, *own)
            for i, one in enumerate(wrapped):
                if staged[i]:
                    one.get()

        return pl.pallas_call(
            body,
            out_shape=values[len(args) :],
            in_specs=[smem] + [hbm if one else vmem for one in staged[: len(args)]],
            out_specs=[hbm if one else vmem for one in staged[len(args) :]],
            scratch_shapes=list(scratch) + buffers + [pltpu.SemaphoreType.DMA((max(1, slots),))],
            compiler_params=pltpu.CompilerParams(vmem_limit_bytes=max(limit, 50) * 1024 * 1024),
            cost_estimate=pl.CostEstimate(
                flops=int(flops), bytes_accessed=int(data_bytes), transcendentals=0
            ),
        )(place, *values[: len(args)])

    return run


def attention_forward_part(images, padded, stream_of, gain, shift, qkv_w, biases, proj_w, norm,
                           qkv, prob, mixed, store):
    norm_ref, qkv_ref, prob_ref, mixed_ref = norm.vmem, qkv.vmem, prob.vmem, mixed.vmem
    width = norm_ref.shape[1]
    pairs = HEADS // 2

    def norm_step(i):
        rows = aligned(i, padded)
        vhat, _ = normalised(stream_of(rows))
        norm_ref[rows, :] = (vhat * gain + shift).astype(BF16)

    image_loop(images, norm_step)
    norm.start()
    qkv_w = qkv_w.get()
    for n in range(6):
        cols = slice(n * 256, (n + 1) * 256)
        part = nn(norm_ref[...], qkv_w[:, cols])
        if n < 2:
            part = part + biases[0:1, cols]
        elif n >= 4:
            part = part + biases[1:2, (n - 4) * 256 : (n - 3) * 256]
        qkv_ref[:, cols] = part.astype(BF16)
    qkv.start()
    masks = half_masks(BF16)

    def heads_step(i):
        rows = aligned(i, padded)
        valid = iota((padded, padded), 1) < SEQ
        for j in range(pairs):
            cols = slice(j * 128, (j + 1) * 128)
            queries = qkv_ref[rows, cols]
            keys = qkv_ref[rows, width + j * 128 : width + (j + 1) * 128]
            values = qkv_ref[rows, 2 * width + j * 128 : 2 * width + (j + 1) * 128]
            total = None
            for h in range(2):
                scores = nt(queries * masks[h], keys) * 0.125
                scores = jnp.where(valid, scores, -1e30)
                shifted = jnp.exp(scores - jnp.max(scores, axis=-1, keepdims=True))
                weights = shifted / jnp.sum(shifted, axis=-1, keepdims=True)
                weights = weights.astype(BF16)
                prob_ref[i * HEADS + 2 * j + h] = weights
                part = nn(weights, values * masks[h])
                total = part if total is None else total + part
            mixed_ref[rows, cols] = total.astype(BF16)

    image_loop(images, heads_step)
    prob.start()
    mixed.start()
    proj_w = proj_w.get()
    for n in range(width // 256):
        cols = slice(n * 256, (n + 1) * 256)
        store(cols, nn(mixed_ref[...], proj_w[:, cols]) + biases[2:3, cols])


def attention_backward_part(images, padded, upstream_ref, stream_of, gain, qkv_w, proj_w, norm_ref, qkv_ref,
                            prob_ref, mixed_ref, low_ref, mixed_grad_ref, joined_ref, proj_out,
                            qkv_out, wide_ref, finish):
    mixed_ref, proj_w = mixed_ref.get(), proj_w.get()
    _, width = mixed_ref.shape
    pairs = HEADS // 2
    low_ref[...] = upstream_ref[...].astype(BF16)
    proj_bias = jnp.sum(low_ref[...].astype(F32), axis=0, keepdims=True)
    for n in range(width // 256):
        cols = slice(n * 256, (n + 1) * 256)
        proj_out[:, cols] = tn(mixed_ref[...], low_ref[:, cols]).astype(BF16)
        mixed_grad_ref[:, cols] = nt(low_ref[...], proj_w[cols, :]).astype(BF16)
    masks = half_masks(BF16)
    qkv_ref, prob_ref = qkv_ref.get(), prob_ref.get()

    def heads_step(i):
        rows = aligned(i, padded)
        for j in range(pairs):
            cols = slice(j * 128, (j + 1) * 128)
            key_cols = slice(width + j * 128, width + (j + 1) * 128)
            value_cols = slice(2 * width + j * 128, 2 * width + (j + 1) * 128)
            queries = qkv_ref[rows, cols]
            keys = qkv_ref[rows, key_cols]
            values = qkv_ref[rows, value_cols]
            grads = mixed_grad_ref[rows, cols]
            query_grad = key_grad = value_grad = None
            for h in range(2):
                low = prob_ref[i * HEADS + 2 * j + h]
                weights = low.astype(F32)
                masked = grads * masks[h]
                weights_grad = nt(masked, values)
                center = jnp.sum(weights * weights_grad, axis=-1, keepdims=True)
                score_grad = (weights * (weights_grad - center)).astype(BF16)
                parts = (
                    nn(score_grad, keys * masks[h]),
                    tn(score_grad, queries * masks[h]),
                    tn(low, masked),
                )
                if query_grad is None:
                    query_grad, key_grad, value_grad = parts
                else:
                    query_grad, key_grad, value_grad = (
                        query_grad + parts[0], key_grad + parts[1], value_grad + parts[2])
            joined_ref[rows, cols] = (query_grad * 0.125).astype(BF16)
            joined_ref[rows, key_cols] = (key_grad * 0.125).astype(BF16)
            joined_ref[rows, value_cols] = value_grad.astype(BF16)

    image_loop(images, heads_step)
    norm_ref, qkv_w = norm_ref.get(), qkv_w.get()
    for n in range(6):
        cols = slice(n * 256, (n + 1) * 256)
        qkv_out[:, cols] = tn(norm_ref[...], joined_ref[:, cols]).astype(BF16)
    for n in range(width // 256):
        cols = slice(n * 256, (n + 1) * 256)
        wide_ref[:, cols] = nt(joined_ref[...], qkv_w[cols, :])
    query_bias = jnp.sum(joined_ref[:, 0:width].astype(F32), axis=0, keepdims=True)
    value_bias = jnp.sum(joined_ref[:, 2 * width :].astype(F32), axis=0, keepdims=True)
    gain_grad, shift_grad = norm_back_part(
        images, padded, wide_ref, stream_of, gain, upstream_ref, finish)
    return gain_grad, shift_grad, query_bias, value_bias, proj_bias


def norm_back_part(images, padded, grad_ref, stream_of, gain, upstream_ref, finish):
    width = grad_ref.shape[1]
    stream_of = stream_of()

    def step(i, carry):
        gain_grad, shift_grad = carry
        rows = aligned(i, padded)
        vhat, inverse = normalised(stream_of(rows))
        grad = grad_ref[rows, :]
        finish(i, rows, upstream_ref[rows, :] + norm_back(grad, gain, vhat, inverse))
        return (
            gain_grad + jnp.sum(grad * vhat, axis=0, keepdims=True),
            shift_grad + jnp.sum(grad, axis=0, keepdims=True),
        )

    zero = jnp.zeros((1, width), F32)
    return lax.fori_loop(0, images, step, (zero, zero))


def rows_of(staged):
    def make():
        ref = staged.get()
        return lambda rows: ref[rows, :].astype(F32)

    return make


def write_shards(me, ways, keep_ref, send_ref, blocks, small=None):
    for r in range(ways):
        target = keep_ref if r % 2 == 0 else send_ref
        shard = lax.bitwise_xor(me, jnp.int32(r))
        at = 0
        for ref, lead in blocks:
            rows = ref.shape[-2] // ways
            window = pl.ds(pl.multiple_of(shard * rows, rows), rows)
            for n in range(ref.shape[-1] // 512):
                cols = slice(n * 512, (n + 1) * 512)
                value = ref[window, cols] if lead is None else ref[lead, window, cols]
                target[r // 2, at : at + rows, :] = value
                at += rows
        if small is not None:
            target[r // 2, at : at + small.shape[0], :] = small


def small_rows(rows, count):
    used = sum(row.shape[0] for row in rows)
    if used < count:
        rows = list(rows) + [jnp.zeros((count - used, rows[0].shape[1]), F32)]
    return jnp.concatenate(rows, axis=0).astype(BF16)


def rank_kernel(groups, local, slots, place, routes, routes_t, grads, rank_te, rank_et, *blocks):
    tokens, experts = rank_te.shape
    me = place[1]
    first = iota((tokens, tokens), 0)
    second = iota((tokens, tokens), 1)
    names = iota((tokens, experts), 1)
    chosen = (routes[:, 0:1] == names) | (routes[:, 1:2] == names)
    chosen = chosen.astype(F32)
    earlier = (second < first).astype(F32).astype(BF16)
    rank_te[...] = jnp.where(chosen > 0, nn(earlier, chosen.astype(BF16)), -1.0)
    names_t = iota((experts, tokens), 0)
    chosen_t = (routes_t[0:1, :] == names_t) | (routes_t[1:2, :] == names_t)
    chosen_t = chosen_t.astype(F32)
    later = (first < second).astype(F32).astype(BF16)
    rank_et[...] = jnp.where(chosen_t > 0, nn(chosen_t.astype(BF16), later), -1.0)
    low = grads[...].astype(BF16)
    slot = iota((slots, tokens), 0).astype(F32)
    for r in range(groups):
        for i in range(local):
            e = lax.bitwise_xor(me, jnp.int32(r)) * local + i
            pick = (rank_et[pl.ds(e, 1), :] == slot).astype(F32).astype(BF16)
            blocks[r][i * slots : (i + 1) * slots, :] = nn(pick, low).astype(BF16)


def forward_kernel(images, padded, groups, local, slots, place, tokens, gains, shifts, qkv_w, biases,
                   proj_w, up_w, up_bias, down_w, gains_two, shifts_two, qkv_two, biases_two, proj_two,
                   router, noise, rank_et,
                   norm_a, qkv_a, prob_a, mixed_a, middle, norm_m, hidden, slope, after_first,
                   norm_b, qkv_b, prob_b, mixed_b, after_attn, moe_norm, probs, *blocks):
    width = tokens.shape[1]
    count = images * padded
    middle_out, first_out, attn_out, moe_out = middle, after_first, after_attn, moe_norm
    middle, after_first, after_attn, moe_norm = [one.vmem for one in (middle, after_first, after_attn, moe_norm)]
    norm_out, hidden_out, slope_out = norm_m, hidden, slope
    norm_m, hidden, slope = norm_m.vmem, hidden.vmem, slope.vmem

    def store_middle(cols, branch):
        middle[:, cols] = tokens[:, cols].astype(F32) + branch

    attention_forward_part(images, padded, lambda rows: tokens[rows, :].astype(F32), gains[0:1, :],
                           shifts[0:1, :], qkv_w, biases, proj_w, norm_a, qkv_a, prob_a, mixed_a,
                           store_middle)

    def norm_step(i):
        rows = aligned(i, padded)
        vhat, _ = normalised(middle[rows, :])
        norm_m[rows, :] = (vhat * gains[1:2, :] + shifts[1:2, :]).astype(BF16)

    middle_out.start()
    image_loop(images, norm_step)
    norm_out.start()
    up_w, down_w = up_w.get(), down_w.get()

    def up_step(n):
        cols = aligned(n, 256)
        pre = nn(norm_m[...], up_w[:, cols]) + up_bias[:, cols]
        value, gradient = gelu_pair(pre)
        hidden[:, cols] = value.astype(BF16)
        slope[:, cols] = gradient.astype(BF16)

    image_loop(up_w.shape[1] // 256, up_step)
    hidden_out.start()
    slope_out.start()
    for n in range(width // 256):
        cols = slice(n * 256, (n + 1) * 256)
        after_first[:, cols] = middle[:, cols] + nn(hidden[...], down_w[:, cols]) + biases[3:4, cols]

    first_out.start()

    def store_after(cols, branch):
        after_attn[:, cols] = after_first[:, cols] + branch

    attention_forward_part(images, padded, lambda rows: after_first[rows, :], gains_two[0:1, :],
                           shifts_two[0:1, :], qkv_two, biases_two, proj_two, norm_b, qkv_b, prob_b,
                           mixed_b, store_after)

    def moe_step(i):
        rows = aligned(i, padded)
        vhat, _ = normalised(after_attn[rows, :])
        moe_norm[rows, :] = (vhat * gains_two[1:2, :] + shifts_two[1:2, :]).astype(BF16)

    attn_out.start()
    image_loop(images, moe_step)
    moe_out.start()
    logits = nn(moe_norm[...], router[...]) + noise[...]
    shifted = jnp.exp(logits - jnp.max(logits, axis=-1, keepdims=True))
    probabilities = shifted / jnp.sum(shifted, axis=-1, keepdims=True)
    probs[...] = probabilities
    high, low = split(probabilities)
    me = place[1]
    slot = iota((slots, count), 0).astype(F32)
    square = (iota((slots, slots), 0) == iota((slots, slots), 1)).astype(F32)
    lanes = iota((slots, router.shape[1]), 1)
    for r in range(groups):
        gates = []
        for i in range(local):
            e = lax.bitwise_xor(me, jnp.int32(r)) * local + i
            pick = (rank_et[pl.ds(e, 1), :] == slot).astype(F32).astype(BF16)
            blocks[r][i * slots : (i + 1) * slots, :] = nn(pick, moe_norm[...]).astype(BF16)
            both = nn(pick, high) + nn(pick, low)
            column = jnp.sum(jnp.where(lanes == e, both, 0.0), axis=1, keepdims=True)
            gates.append(jnp.sum(square * column, axis=0, keepdims=True))
        put_scalars(blocks[r], local * slots, gates, slots)


def put_scalars(ref, at, rows, slots):
    parts = []
    for row in rows:
        high, low = split(row)
        parts += [high.astype(F32), low.astype(F32)]
    parts.append(jnp.zeros((EXTRA - len(parts), slots), F32))
    ref[at : at + EXTRA, :] = jnp.zeros((EXTRA, ref.shape[1]), BF16)
    ref[at : at + EXTRA, 0:slots] = jnp.concatenate(parts, axis=0).astype(BF16)


def scalar_row(ref, at, i, slots):
    block = ref[at : at + EXTRA, 0:slots].astype(F32)
    return block[2 * i : 2 * i + 1, :] + block[2 * i + 1 : 2 * i + 2, :]


def early_kernel(groups, local, slots, place, out_w, *refs):
    blocks, staged = refs[:groups], refs[groups]
    product = staged.vmem
    for i in range(local):
        out_ref = out_w.get(i)
        for r in range(groups):
            rows = blocks[r][i * slots : (i + 1) * slots, :]
            for n in range(4):
                cols = slice(n * 512, (n + 1) * 512)
                product[i, r * slots : (r + 1) * slots, cols] = nt(rows, out_ref[i, cols, :]).astype(BF16)
        staged.start(i)


def expert_kernel(groups, local, slots, place, in_w, in_bias, out_bias, product, *refs):
    rows_in, grads_in = refs[:groups], refs[groups : 2 * groups]
    blocks, hidden_out, low_out = refs[2 * groups : 3 * groups], refs[3 * groups], refs[3 * groups + 1]
    hidden, low = hidden_out.vmem, low_out.vmem
    staged_w, staged_product = in_w, product
    joined = refs[3 * groups + 2]
    square = (iota((slots, slots), 0) == iota((slots, slots), 1)).astype(F32)
    scalars = [[] for _ in range(groups)]
    for i in range(local):
        in_w, product = staged_w.get(i), staged_product.get(i)
        for r in range(groups):
            joined[r * slots : (r + 1) * slots, :] = rows_in[r][i * slots : (i + 1) * slots, :]

        def up_step(n, total):
            cols = aligned(n, 256)
            pre = nn(joined[...], in_w[i, :, cols]) + in_bias[i : i + 1, cols]
            value, gradient = gelu_pair(pre)
            value = value.astype(BF16)
            hidden[i, :, cols] = value
            scale = product[i, :, cols].astype(F32)
            low[i, :, cols] = (scale * gradient).astype(BF16)
            both = value.astype(F32) * scale
            return total + both[:, 0:128] + both[:, 128:256]

        total = lax.fori_loop(0, in_w.shape[2] // 256, up_step, jnp.zeros((groups * slots, 128), F32))
        hidden_out.start(i)
        low_out.start(i)
        total = jnp.sum(total, axis=1, keepdims=True)
        for r in range(groups):
            g_rows = grads_in[r][i * slots : (i + 1) * slots, :].astype(F32)
            extra = jnp.sum(g_rows * out_bias[i : i + 1, :], axis=1, keepdims=True)
            column = total[r * slots : (r + 1) * slots, :] + extra
            scalars[r].append(jnp.sum(square * column, axis=0, keepdims=True))
        for n in range(2):
            cols = slice(n * 256, (n + 1) * 256)
            back = nt(low[i], in_w[i, cols, :]).astype(BF16)
            for r in range(groups):
                blocks[r][i * slots : (i + 1) * slots, cols] = back[r * slots : (r + 1) * slots, :]
    for r in range(groups):
        put_scalars(blocks[r], local * slots, scalars[r], slots)


def value_kernel(groups, local, slots, place, hidden_in, out_in, out_bias, *blocks):
    for i in range(local):
        hidden, out_w = hidden_in.get(i), out_in.get(i)
        for n in range(2):
            cols = slice(n * 256, (n + 1) * 256)
            value = nn(hidden[i], out_w[i, :, cols]) + out_bias[i : i + 1, cols]
            value = value.astype(BF16)
            for r in range(groups):
                blocks[r][i * slots : (i + 1) * slots, cols] = value[r * slots : (r + 1) * slots, :]


def weight_kernel(groups, local, slots, ways, place, low_in, hidden_in, *refs):
    rows_in, grads_in = refs[:groups], refs[groups : 2 * groups]
    keep, send = refs[2 * groups], refs[2 * groups + 1]
    scaled, value_grad, in_out, out_out = refs[2 * groups + 2 :]
    square = (iota((slots, slots), 0) == iota((slots, slots), 1)).astype(F32)
    small = []
    tail = []
    for i in range(local):
        low, hidden = low_in.get(i), hidden_in.get(i)
        gate_rows = []
        for r in range(groups):
            gate = scalar_row(rows_in[r], local * slots, i, slots)
            gate_rows.append(gate)
            column = jnp.sum(square * gate, axis=1, keepdims=True)
            own = slice(i * slots, (i + 1) * slots)
            at = slice(r * slots, (r + 1) * slots)
            scaled[at, :] = (rows_in[r][own, :].astype(F32) * column).astype(BF16)
            value_grad[at, :] = (grads_in[r][own, :].astype(F32) * column).astype(BF16)
        bias_parts = []
        for n in range(4):
            cols = slice(n * 512, (n + 1) * 512)
            in_out[i, :, cols] = tn(scaled[...], low[i, :, cols]).astype(BF16)
            total = jnp.zeros((8, 512), F32)
            for r in range(groups):
                high, rest = split(jnp.broadcast_to(gate_rows[r], (8, slots)))
                piece = low[i, r * slots : (r + 1) * slots, cols]
                total = total + nn(high, piece) + nn(rest, piece)
            bias_parts.append(total[0:1, :])
            out_out[i, cols, :] = tn(hidden[i, :, cols], value_grad[...]).astype(BF16)
        small += bias_parts
        tail.append(jnp.sum(value_grad[...].astype(F32), axis=0, keepdims=True))
    blocks = []
    for i in range(local):
        blocks += [(in_out, i), (out_out, i)]
    write_shards(place[0], ways, keep, send, blocks, small_rows(small + tail, 16))


def combine_columns(rank_te, probs, e, slots):
    tokens, experts = rank_te.shape
    mask = iota((tokens, experts), 1) == e
    column = jnp.sum(jnp.where(mask, rank_te[...], 0.0), axis=1, keepdims=True)
    gate = jnp.sum(jnp.where(mask, probs[...], 0.0), axis=1, keepdims=True)
    pick = (column == iota((tokens, slots), 1).astype(F32)).astype(F32)
    return mask, pick, gate


def output_kernel(groups, local, slots, place, rank_te, probs, after_attn, *refs):
    blocks, out, total = refs[:groups], refs[groups], refs[groups + 1]
    total[...] = after_attn[...]
    for r in range(groups):
        for i in range(local):
            e = lax.bitwise_xor(place[1], jnp.int32(r)) * local + i
            _, pick, gate = combine_columns(rank_te, probs, e, slots)
            total[...] += gate * nn(pick.astype(BF16), blocks[r][i * slots : (i + 1) * slots, :])
    out[...] = total[...].astype(BF16)


def attn_two_kernel(images, padded, groups, local, slots, ways, small_count, place, rank_te, probs,
                    after_attn, grads, gains, shifts, router, moe_norm, after_first, qkv_w, proj_w, norm_b,
                    qkv_b, prob_b, mixed_b, *refs):
    blocks = refs[:groups]
    stream_grad, keep, send, small_out = refs[groups : groups + 4]
    moe_norm, grads_in, attn_in, first_in = moe_norm.get(), grads, after_attn, after_first
    wide, upstream, low_ref, mixed_grad, joined, proj_out, qkv_out = refs[groups + 4 :]
    tokens, experts = rank_te.shape
    wide[...] = jnp.zeros_like(wide)
    gate_grad = jnp.zeros((tokens, experts), F32)
    for r in range(groups):
        for i in range(local):
            e = lax.bitwise_xor(place[1], jnp.int32(r)) * local + i
            mask, pick, gate = combine_columns(rank_te, probs, e, slots)
            scalars = scalar_row(blocks[r], local * slots, i, slots)
            column = jnp.sum(pick * scalars, axis=1, keepdims=True)
            gate_grad = jnp.where(mask, column, gate_grad)
            wide[...] += gate * nn(pick.astype(BF16), blocks[r][i * slots : (i + 1) * slots, :])
    probabilities = probs[...]
    inner = jnp.sum(probabilities * gate_grad, axis=1, keepdims=True)
    logit_grad = probabilities * (gate_grad - inner)
    high, rest = split(logit_grad)
    router_grad = tn(high, moe_norm[...]) + tn(rest, moe_norm[...])
    wide[...] += nt(high, router[...]) + nt(rest, router[...])

    def finish_moe(i, rows, value):
        upstream[rows, :] = value

    moe_gain, moe_shift = norm_back_part(images, padded, wide, rows_of(attn_in), gains[1:2, :],
                                         grads_in.get(), finish_moe)

    def finish(i, rows, value):
        stream_grad[rows, :] = value

    sums = attention_backward_part(images, padded, upstream, rows_of(first_in),
                                   gains[0:1, :], qkv_w, proj_w, norm_b, qkv_b, prob_b, mixed_b, low_ref,
                                   mixed_grad, joined, proj_out, qkv_out, wide, finish)
    gain_grad, shift_grad, query_bias, value_bias, proj_bias = sums
    small_out[...] = small_rows([gain_grad, moe_gain, shift_grad, moe_shift, query_bias, value_bias,
                                 proj_bias, router_grad], small_count)
    write_shards(place[0], ways, keep, send, [(qkv_out, None), (proj_out, None)])


def mlp_back_kernel(images, padded, ways, place, upstream, slope, down_w, hidden, norm_m, up_w, middle,
                    gains, stream_grad, keep, send, small_out, low_ref, pre_grad, up_out, down_out, wide):
    width = upstream.shape[1]
    middle_in, up_in = middle, up_w
    low_ref[...] = upstream[...].astype(BF16)
    slope, down_w, hidden, norm_m = slope.get(), down_w.get(), hidden.get(), norm_m.get()
    down_bias = jnp.sum(low_ref[...].astype(F32), axis=0, keepdims=True)
    bias_parts = []
    for n in range(4):
        cols = slice(n * 512, (n + 1) * 512)
        hidden_grad = nt(low_ref[...], down_w[cols, :])
        value = (hidden_grad * slope[:, cols].astype(F32)).astype(BF16)
        pre_grad[:, cols] = value
        bias_parts.append(jnp.sum(value.astype(F32), axis=0, keepdims=True))
        down_out[cols, :] = tn(hidden[:, cols], low_ref[...]).astype(BF16)
        up_out[:, cols] = tn(norm_m[...], value).astype(BF16)
    up_w = up_in.get()
    for n in range(width // 256):
        cols = slice(n * 256, (n + 1) * 256)
        wide[:, cols] = nt(pre_grad[...], up_w[cols, :])

    def finish(i, rows, value):
        stream_grad[rows, :] = value

    gain_grad, shift_grad = norm_back_part(images, padded, wide, rows_of(middle_in), gains[1:2, :],
                                           upstream, finish)
    small_out[...] = small_rows([gain_grad, shift_grad, down_bias] + bias_parts, 16)
    write_shards(place[0], ways, keep, send, [(up_out, None), (down_out, None)])


def attn_one_kernel(images, padded, ways, place, upstream, mixed_a, proj_w, qkv_a, prob_a, norm_a, qkv_w,
                    tokens, gains, small_two, small_mlp, stream_grad, keep, send, low_ref, mixed_grad, joined, proj_out,
                    qkv_out, wide):
    def finish(i, rows, value):
        stream_grad[rows, :] = value

    sums = attention_backward_part(images, padded, upstream, rows_of(tokens),
                                   gains[0:1, :], qkv_w, proj_w, norm_a, qkv_a, prob_a, mixed_a, low_ref,
                                   mixed_grad, joined, proj_out, qkv_out, wide, finish)
    filled = 4 * (qkv_out.shape[0] // ways)
    rest = keep.shape[1] - filled - 16 - small_two.shape[0] - small_mlp.shape[0]
    parts = [small_rows(sums, 16), small_two[...], small_mlp[...]]
    if rest:
        parts.append(jnp.zeros((rest, small_two.shape[1]), BF16))
    small = jnp.concatenate(parts, axis=0)
    write_shards(place[0], ways, keep, send, [(qkv_out, None), (proj_out, None)], small)


def bit_count(value):
    return value.bit_length() - 1


def flip(index, bit):
    step = 1 << bit
    return index + (1 - 2 * ((index // step) % 2)) * step


def reduce_kernel(chunks, ways, groups, *refs):
    sources = max(source for source, _ in chunks) + 1
    keeps, sends, outs = [[refs[kind * sources + k] for k in range(sources)] for kind in range(3)]
    scratch = refs[3 * sources :]
    send_sems, recv_sems = scratch[-2], scratch[-1]
    places = ways // 2
    plane_bits, group_bits = bit_count(places), bit_count(groups)
    half = groups // 2
    md, mz = lax.axis_index("dp"), lax.axis_index("expert")
    partners = [{"dp": flip(md, b)} for b in range(plane_bits + 1)]
    partners += [{"expert": flip(mz, b)} for b in range(group_bits)]

    def send_to(src, dst, sem, partner):
        copy = pltpu.make_async_remote_copy(
            src_ref=src, dst_ref=dst, send_sem=send_sems.at[sem], recv_sem=recv_sems.at[sem],
            device_id=partner, device_id_type=pl.DeviceIdType.MESH)
        copy.start()
        return copy

    barrier = pltpu.get_barrier_semaphore()
    for partner in partners:
        pl.semaphore_signal(barrier, inc=1, device_id=partner, device_id_type=pl.DeviceIdType.MESH)
    pl.semaphore_wait(barrier, len(partners))

    def over(count, body):
        def step(i, carry):
            body(i)
            return carry

        lax.fori_loop(0, count, step, 0)

    def chunk_steps(c):
        source, first = chunks[c]
        keep, send, out = keeps[source], sends[source], outs[source]
        core_in, low, total, plane_in, group_low, group_in, gathered = scratch[7 * c : 7 * c + 7]
        per_chunk = send_sems.shape[0] // len(chunks)
        used = [c * per_chunk]
        live = []

        def go(src, dst, partner):
            live.append(send_to(src, dst, used[0], partner))
            used[0] += 1

        def core_start():
            go(send.at[:, pl.ds(first, groups)], core_in, partners[0])

        def plane_start(step):
            for h in range(2):
                bit = step if h == 0 else plane_bits - 1 - step
                sent = sum(places >> (t + 1) for t in range(step))
                parts = pl.ds(h * half, half)
                for j in plane_active(h, step):
                    if (j >> bit) & 1:
                        go(low.at[j, parts], plane_in.at[h, sent], partners[1 + bit])
                        sent += 1

        def plane_active(h, step):
            done = 0
            for t in range(step):
                done |= 1 << (t if h == 0 else plane_bits - 1 - t)
            return [j for j in range(places) if not j & done]

        def plane_finish(step):
            for h in range(2):
                bit = step if h == 0 else plane_bits - 1 - step
                at = sum(places >> (t + 1) for t in range(step))
                for j in plane_active(h, step):
                    if not (j >> bit) & 1:
                        def add(i, j=j, at=at, h=h):
                            part = h * half + i
                            value = plane_in[h, at, i].astype(F32)
                            if j == 0:
                                total[part] = total[part] + value
                            else:
                                low[j, part] = (low[j, part].astype(F32) + value).astype(BF16)

                        over(half, add)
                        at += 1

        def core_finish():
            def add(i):
                for j in range(places):
                    value = keep[j, first + i].astype(F32) + core_in[j, i].astype(F32)
                    if j == 0:
                        total[i] = value
                    else:
                        low[j, i] = value.astype(BF16)

            over(groups, add)

        def group_start(bit):
            step = 1 << bit
            base = mz % step + step * (1 - (mz // step) % 2)
            at = sum(groups >> (b + 1) for b in range(bit))
            for u in range(groups // (2 * step)):
                go(group_low.at[base + 2 * step * u], group_in.at[at + u], partners[1 + plane_bits + bit])

        def group_finish(bit):
            step = 1 << bit
            base = mz % step + step * ((mz // step) % 2)
            at = sum(groups >> (b + 1) for b in range(bit))
            for u in range(groups // (2 * step)):
                part = base + 2 * step * u
                value = total[part] + group_in[at + u].astype(F32)
                total[part] = value
                group_low[part] = value.astype(BF16)

        def gather_start(bit):
            step = 2 << bit
            base = mz % step
            for u in range(groups // step):
                part = base + step * u
                go(gathered.at[part], gathered.at[part], partners[1 + plane_bits + bit])

        def settle():
            for copy in live:
                copy.wait()
            live.clear()

        phases = []

        def phase(start, finish):
            phases.append((start, finish))

        phase(core_start, core_finish)
        for step in range(plane_bits):
            phase(functools.partial(plane_start, step), functools.partial(plane_finish, step))

        def to_low():
            over(groups, lambda i: group_low.__setitem__(i, total[i].astype(BF16)))

        for bit in range(group_bits):
            def start(bit=bit):
                if bit == 0:
                    to_low()
                group_start(bit)

            phase(start, functools.partial(group_finish, bit))
        for bit in reversed(range(group_bits)):
            def start(bit=bit):
                if bit == group_bits - 1:
                    gathered[mz] = group_low[mz]
                gather_start(bit)

            phase(start, lambda: None)

        def write():
            over(groups, lambda i: out.__setitem__(first + i, gathered[i].astype(F32)))

        return phases, settle, write

    built = [chunk_steps(c) for c in range(len(chunks))]
    for phases, _, _ in built:
        phases[0][0]()
    count = len(built[0][0])
    slot_of = [0] + [index + 1 for index in range(1, count)]
    for slot in range(len(built) + count):
        for c, (phases, settle, write) in enumerate(built):
            for index in range(count):
                if slot_of[index] + c == slot:
                    settle()
                    phases[index][1]()
                    if index + 1 < count:
                        phases[index + 1][0]()
                    else:
                        write()


def reduce_all(pairs, chunks, ways, groups):
    vmem = pl.BlockSpec(memory_space=pltpu.VMEM)
    places = ways // 2
    scratch = []
    for source, _ in chunks:
        rows = pairs[source][0].shape[2]
        scratch += [
            pltpu.VMEM((places, groups, rows, 512), BF16), pltpu.VMEM((places, groups, rows, 512), BF16),
            pltpu.VMEM((groups, rows, 512), F32), pltpu.VMEM((2, places - 1, groups // 2, rows, 512), BF16),
            pltpu.VMEM((groups, rows, 512), BF16), pltpu.VMEM((groups - 1, rows, 512), BF16),
            pltpu.VMEM((groups, rows, 512), BF16)]
    count = len(chunks) * (1 + 2 * (places - 1) + 2 * (groups - 1))
    outs = [jax.ShapeDtypeStruct(keep.shape[1:], F32) for keep, _ in pairs]
    return pl.pallas_call(
        functools.partial(reduce_kernel, chunks, ways, groups),
        out_shape=outs,
        in_specs=[vmem] * (2 * len(pairs)),
        out_specs=[vmem] * len(outs),
        scratch_shapes=scratch + [pltpu.SemaphoreType.DMA((count,)), pltpu.SemaphoreType.DMA((count,))],
        compiler_params=pltpu.CompilerParams(
            collective_id=0, has_side_effects=True, vmem_limit_bytes=48 * 1024 * 1024),
        cost_estimate=pl.CostEstimate(flops=10**7, bytes_accessed=10**8, transcendentals=0),
        name="reduce",
    )(*[keep for keep, _ in pairs], *[send for _, send in pairs])


def exchange(value, axis, mask):
    size = lax.axis_size(axis)
    return lax.ppermute(value, axis, [(i, i ^ mask) for i in range(size)])


def spread(blocks):
    return [blocks[0]] + [exchange(blocks[r], "expert", r) for r in range(1, len(blocks))]


def core_sum(keep, send, ways):
    arrived = exchange(send, "dp", 1)
    sums = [keep[j].astype(F32) + arrived[j].astype(F32) for j in range(ways // 2)]
    return (sums[0],) + tuple(value.astype(BF16) for value in sums[1:])


def plane_start(sums, ways):
    return tuple(exchange(sums[j], "dp", 2 * j) for j in range(1, ways // 2))


def plane_sum(sums, parts):
    total = sums[0]
    for part in parts:
        total = total + part.astype(F32)
    return total


def columns_of(rows, me, ways):
    share = rows.shape[1] // ways
    return lax.dynamic_slice_in_dim(rows, me * share, share, axis=1)


def joined_blocks(total, at, rows, count):
    parts = [total[at + n * rows : at + (n + 1) * rows, :] for n in range(count)]
    return jnp.concatenate(parts, axis=1), at + count * rows


def per_device(tokens, cotangent, dense_gains, dense_shifts, dense_qkv, dense_biases, dense_proj, dense_up,
               dense_up_bias, dense_down, moe_gains, moe_shifts, moe_qkv, moe_biases, moe_proj, router,
               router_noise, routes, expert_in, expert_in_bias, expert_out, expert_out_bias):
    count, width = tokens.shape
    top = routes.shape[1]
    experts = router.shape[1]
    groups = lax.axis_size("expert")
    ways = lax.axis_size("dp")
    local = expert_in.shape[0]
    ff = dense_up.shape[1]
    images = count // SEQ
    padded = round_up(SEQ, 16)
    full = images * padded
    capacity = max(2, (5 * count * top + 4 * experts - 1) // (4 * experts))
    slots = round_up(capacity, 16)
    me = lax.axis_index("dp").astype(jnp.int32)
    place = jnp.stack([me, lax.axis_index("expert").astype(jnp.int32)])

    def pad(array, value=0):
        shaped = array.reshape(images, SEQ, array.shape[1])
        shaped = jnp.pad(shaped, ((0, 0), (0, padded - SEQ), (0, 0)), constant_values=value)
        return shaped.reshape(full, array.shape[1])

    def unpad(array):
        return array.reshape(images, padded, width)[:, :SEQ, :].reshape(count, width)

    def shape(*dims, dtype=BF16):
        return jax.ShapeDtypeStruct(dims, dtype)

    tokens_p = pad(tokens)
    grads_p = pad(cotangent)
    noise_p = pad(router_noise)
    routes_p = pad(routes, -1)
    matmul = 2 * full * width

    row_block = local * slots
    ranks = call(
        functools.partial(rank_kernel, groups, local, slots),
        [shape(full, experts, dtype=F32), shape(experts, full, dtype=F32)]
        + [shape(row_block, width)] * groups,
        [], 2 * groups * row_block * full * width, 8e6, 24,
    )(place, routes_p, routes_p.T, grads_p)
    rank_te, rank_et, grad_blocks = ranks[0], ranks[1], ranks[2:]
    grad_blocks = spread(grad_blocks)

    forward = call(
        functools.partial(forward_kernel, images, padded, groups, local, slots),
        [Hbm(one) for one in
         (shape(full, width), shape(full, 3 * width), shape(images * HEADS, padded, padded),
          shape(full, width), shape(full, width, dtype=F32), shape(full, width), shape(full, ff),
          shape(full, ff), shape(full, width, dtype=F32), shape(full, width), shape(full, 3 * width),
          shape(images * HEADS, padded, padded), shape(full, width), shape(full, width, dtype=F32),
          shape(full, width))] + [shape(full, experts, dtype=F32)]
        + [shape(row_block + EXTRA, width)] * groups,
        [], matmul * (8 * width + 2 * ff), 30e6, 44,
    )(place, tokens_p, dense_gains, dense_shifts, Hbm(dense_qkv), dense_biases, Hbm(dense_proj), Hbm(dense_up),
      dense_up_bias.reshape(1, ff), Hbm(dense_down), moe_gains, moe_shifts, Hbm(moe_qkv), moe_biases,
      Hbm(moe_proj), router, noise_p, rank_et)
    (norm_a, qkv_a, prob_a, mixed_a, middle, norm_m, hidden, slope, after_first, norm_b, qkv_b, prob_b,
     mixed_b, after_attn, moe_norm, probs) = forward[:16]
    rows_out = forward[16:]
    row_blocks = spread(rows_out)

    total_rows = groups * slots
    expert_flops = 2 * local * total_rows * width * ff
    product, = call(
        functools.partial(early_kernel, groups, local, slots), [Hbm(shape(local, total_rows, ff), local)], [],
        expert_flops, 12e6, 20,
    )(place, Hbm(expert_out, local), *grad_blocks)
    expert = call(
        functools.partial(expert_kernel, groups, local, slots),
        [shape(row_block + EXTRA, width)] * groups
        + [Hbm(shape(local, total_rows, ff), local)] * 2,
        [pltpu.VMEM((total_rows, width), BF16)], 2 * expert_flops, 25e6, 36,
    )(place, Hbm(expert_in, local), expert_in_bias, expert_out_bias, Hbm(product, local), *row_blocks,
      *grad_blocks)
    back_out, expert_hidden, expert_low = expert[:groups], expert[groups], expert[groups + 1]
    back_blocks = spread(back_out)

    shard_rows = local * (width // ways * (ff // 512) + ff // ways) + 16
    keep, send = call(
        functools.partial(weight_kernel, groups, local, slots, ways),
        [shape(ways // 2, shard_rows, 512)] * 2,
        [pltpu.VMEM((total_rows, width), BF16), pltpu.VMEM((total_rows, width), BF16),
         pltpu.VMEM((local, width, ff), BF16), pltpu.VMEM((local, ff, width), BF16)],
        2 * expert_flops, 25e6, 44,
    )(place, Hbm(expert_low, local), Hbm(expert_hidden, local), *row_blocks, *grad_blocks)
    expert_hidden, keep, send = lax.optimization_barrier((expert_hidden, keep, send))
    value_out = call(
        functools.partial(value_kernel, groups, local, slots), [shape(row_block, width)] * groups, [],
        expert_flops, 12e6, 20,
    )(place, Hbm(expert_hidden, local), Hbm(expert_out, local), expert_out_bias)
    expert_sums = core_sum(keep, send, ways)
    value_out, back_blocks, expert_sums, rank_te = lax.optimization_barrier(
        (tuple(value_out), tuple(back_blocks), expert_sums, rank_te))
    value_blocks = spread(value_out)
    expert_parts = plane_start(expert_sums, ways)

    attn_scratch = [pltpu.VMEM((full, width), BF16), pltpu.VMEM((full, width), BF16),
                    pltpu.VMEM((full, 3 * width), BF16), pltpu.VMEM((width, width), BF16),
                    pltpu.VMEM((width, 3 * width), BF16)]
    wide = pltpu.VMEM((full, width), F32)
    small_two = round_up(7 + experts, 16)
    attn_rows = width // ways * 4
    mlp_rows = width // ways * (ff // 512) + ff // ways
    one_rows = round_up(attn_rows + 32 + small_two, 16 * groups)
    grad_first, two_keep, two_send, two_small = call(
        functools.partial(attn_two_kernel, images, padded, groups, local, slots, ways, small_two),
        [shape(full, width, dtype=F32)] + [shape(ways // 2, attn_rows, 512)] * 2 + [shape(small_two, 512)],
        [wide, wide] + attn_scratch, matmul * 12 * width, 20e6, 30,
    )(place, rank_te, probs, Hbm(after_attn), Hbm(grads_p), moe_gains, moe_shifts, router, Hbm(moe_norm),
      Hbm(after_first), Hbm(moe_qkv), Hbm(moe_proj), Hbm(norm_b), Hbm(qkv_b), Hbm(prob_b), Hbm(mixed_b),
      *back_blocks)

    grad_middle, mlp_keep, mlp_send, mlp_small = call(
        functools.partial(mlp_back_kernel, images, padded, ways),
        [shape(full, width, dtype=F32)] + [shape(ways // 2, mlp_rows, 512)] * 2 + [shape(16, 512)],
        [pltpu.VMEM((full, width), BF16), pltpu.VMEM((full, ff), BF16), pltpu.VMEM((width, ff), BF16),
         pltpu.VMEM((ff, width), BF16), wide],
        matmul * 4 * ff, 20e6, 36,
    )(place, grad_first, Hbm(slope), Hbm(dense_down), Hbm(hidden), Hbm(norm_m), Hbm(dense_up), Hbm(middle),
      dense_gains)

    token_grad, one_keep, one_send = call(
        functools.partial(attn_one_kernel, images, padded, ways),
        [shape(full, width, dtype=F32)] + [shape(ways // 2, one_rows, 512)] * 2,
        attn_scratch + [wide], matmul * 10 * width, 20e6, 26,
    )(place, grad_middle, Hbm(mixed_a), Hbm(dense_proj), Hbm(qkv_a), Hbm(prob_a), Hbm(norm_a), Hbm(dense_qkv),
      Hbm(tokens_p), dense_gains, two_small, mlp_small)

    def in_parts(array):
        rows = array.shape[1]
        size = rows // groups if rows < 2 * attn_rows else rows // (2 * groups)
        return array.reshape(ways // 2, rows // size, size, 512)

    pairs = [(in_parts(two_keep), in_parts(two_send)), (in_parts(mlp_keep), in_parts(mlp_send)),
             (in_parts(one_keep), in_parts(one_send))]
    totals = reduce_all(pairs, ((0, 0), (1, 0), (1, groups), (2, 0)), ways, groups)
    two_total, mlp_total, one_total = [total.reshape(-1, 512) for total in totals]
    expert_total = plane_sum(expert_sums, expert_parts)

    out_tokens, = call(
        functools.partial(output_kernel, groups, local, slots), [shape(full, width)],
        [wide], 2 * experts * slots * full * width, 5e6, 20,
    )(place, rank_te, probs, after_attn, *value_blocks)

    share = width // ways
    small = one_total[attn_rows : attn_rows + 16]
    two_small = one_total[attn_rows + 16 : attn_rows + 16 + small_two]
    mlp_small = one_total[attn_rows + 16 + small_two : attn_rows + 32 + small_two]
    dense_qkv_grad, at = joined_blocks(one_total, 0, share, 3)
    dense_proj_grad = one_total[at : at + share]
    dense_up_grad, at = joined_blocks(mlp_total, 0, share, ff // 512)
    dense_down_grad = mlp_total[at : at + ff // ways]
    moe_qkv_grad, at = joined_blocks(two_total, 0, share, 3)
    moe_proj_grad = two_total[at : at + share]
    gains_one = columns_of(jnp.stack([small[0], mlp_small[0]]), me, ways)
    shifts_one = columns_of(jnp.stack([small[1], mlp_small[1]]), me, ways)
    biases_one = columns_of(jnp.stack([small[2], small[3], small[4], mlp_small[2]]), me, ways)
    up_bias_grad = columns_of(mlp_small[3 : 3 + ff // 512].reshape(1, ff), me, ways).reshape(-1)
    two_cols = columns_of(two_small, me, ways)
    router_grad = two_cols[7 : 7 + experts].T
    in_grads, out_grads = [], []
    at = 0
    for _ in range(local):
        part, at = joined_blocks(expert_total, at, share, ff // 512)
        in_grads.append(part)
        out_grads.append(expert_total[at : at + ff // ways])
        at += ff // ways
    expert_small = expert_total[at:]
    in_bias = columns_of(expert_small[0 : local * (ff // 512)].reshape(local, ff), me, ways)
    out_bias = columns_of(expert_small[local * (ff // 512) : local * (ff // 512) + local], me, ways)
    return (
        unpad(out_tokens), unpad(token_grad), gains_one, shifts_one, dense_qkv_grad, biases_one,
        dense_proj_grad, dense_up_grad, up_bias_grad, dense_down_grad, two_cols[0:2], two_cols[2:4],
        moe_qkv_grad, two_cols[4:7], moe_proj_grad, router_grad, jnp.stack(in_grads), in_bias,
        jnp.stack(out_grads), out_bias,
    )


def solution(mesh):
    rows = P(("dp", "expert"), None)
    placed = (rows, rows) + (P(),) * 14 + (
        rows, rows, P("expert", None, None), P("expert", None), P("expert", None, None), P("expert", None))
    col, row = P(None, "dp"), P("dp", None)
    return jax.shard_map(
        per_device,
        mesh=mesh,
        in_specs=placed,
        out_specs=(
            rows, rows, col, col, row, col, row, row, P("dp"), row, col, col, row, col, row, row,
            P("expert", "dp", None), P("expert", "dp"), P("expert", "dp", None), P("expert", "dp")),
        check_vma=False,
    )
```
